32 devices in a mesh: dp: 1 (over z), tp2: 4 (over y), tp: 8 (over x, core).
Axes of the slice: x: 4, y: 4, z: 1, core: 2. Of those that a mesh axis runs over, the one named last changes fastest.
The devices are a block of a 4x4x8 slice.
Arguments:
- hidden: bfloat16 [512, 5120], P('dp')
- w_gate: bfloat16 [5120, 13824], P(None, ('tp', 'tp2'))
- w_up: bfloat16 [5120, 13824], P(None, ('tp', 'tp2'))
- w_down: bfloat16 [13824, 5120], P('tp', 'tp2')
- norm_gain: float32 [5120], replicated
- w_vocab: bfloat16 [5120, 32000], P('tp2', 'tp')
- temperature: float32 [512], P('dp')
- target: int32 [512], P('dp')
Outputs:
- output 1: float32 [512], P('dp')
- output 2: float32 [512], P('dp')
- output 3: float32 [512], P('dp')
- output 4: bfloat16 [512, 32000], P('dp', ('tp', 'tp2'))
All inputs are finite; a program needn't handle non-finite values.
Results may differ from the reference program's by a relative error of at most 0.00765.
Values are sent between devices in bfloat16 or wider.
A program may use at most 768 MiB of HBM per device.

```python
import jax
import jax.numpy as jnp
from jax import lax

B = 512
D = 5120
FF = 13824
V = 32000
ROW_BLOCK = 8
NORM_EPS = 1e-6


def setup_inputs(seed: int = 0, part: int = 0) -> dict:
    base_key = jax.random.key(seed)
    shared = jax.random.split(base_key, 5)
    own_keys = jax.random.split(jax.random.fold_in(base_key, part), 5)
    hidden = jax.random.normal(own_keys[0], (B, D), jnp.float32).astype(jnp.bfloat16)
    w_gate = (jax.random.normal(shared[0], (D, FF), jnp.float32) * D ** -0.5).astype(jnp.bfloat16)
    w_up = (jax.random.normal(shared[1], (D, FF), jnp.float32) * D ** -0.5).astype(jnp.bfloat16)
    w_down = (jax.random.normal(shared[2], (FF, D), jnp.float32) * (1.6 * FF ** -0.5)).astype(jnp.bfloat16)
    norm_gain = jax.random.uniform(shared[3], (D,), jnp.float32, 0.5, 1.5)
    w_vocab = (jax.random.normal(shared[4], (D, V), jnp.float32) * (2.5 * D ** -0.5)).astype(jnp.bfloat16)
    temperature = jax.random.uniform(own_keys[1], (B,), jnp.float32, 0.5, 2.0)
    raw_target = jax.random.randint(own_keys[2], (B,), 0, V, jnp.int32)
    first_row = jax.random.randint(own_keys[3], (), 0, B, jnp.int32)
    second_row = (first_row + 1 + jax.random.randint(own_keys[4], (), 0, B - 1, jnp.int32)) % B
    row_ids = jnp.arange(B, dtype=jnp.int32)
    target = jnp.where(row_ids == first_row, 0, jnp.where(row_ids == second_row, V - 1, raw_target)).astype(jnp.int32)
    return {'hidden': hidden, 'w_gate': w_gate, 'w_up': w_up, 'w_down': w_down, 'norm_gain': norm_gain, 'w_vocab': w_vocab, 'temperature': temperature, 'target': target}


def reference(hidden, w_gate, w_up, w_down, norm_gain, w_vocab, temperature, target):
    gate_pre = jnp.dot(hidden, w_gate, preferred_element_type=jnp.float32)
    up_pre = jnp.dot(hidden, w_up, preferred_element_type=jnp.float32)
    act_rows = (jax.nn.silu(gate_pre) * up_pre).astype(jnp.bfloat16)
    y_rows = jnp.dot(act_rows, w_down, preferred_element_type=jnp.float32)
    residual = hidden.astype(jnp.float32) + y_rows
    inv_rms = lax.rsqrt(jnp.mean(residual * residual, axis=1, keepdims=True) + NORM_EPS)
    normed = (norm_gain * residual * inv_rms).astype(jnp.bfloat16)
    num_blocks = B // ROW_BLOCK
    col_ids = jnp.arange(V, dtype=jnp.int32)[None, :]

    def head_block(block_args):
        x_blk, temp_blk, tgt_blk = block_args
        logits = jnp.dot(x_blk, w_vocab, preferred_element_type=jnp.float32) / temp_blk[:, None]
        row_max = jnp.max(logits, axis=1)
        exp_shift = jnp.exp(logits - row_max[:, None])
        sum_exp = jnp.sum(exp_shift, axis=1)
        log_norm = row_max + jnp.log(sum_exp)
        entropy = log_norm - jnp.sum(exp_shift * logits, axis=1) / sum_exp
        tgt_logit = jnp.sum(jnp.where(col_ids == tgt_blk[:, None], logits, 0.0), axis=1)
        logprobs = (logits - log_norm[:, None]).astype(jnp.bfloat16)
        return log_norm, entropy, tgt_logit - log_norm, logprobs

    log_norm, entropy, tgt_logp, logprobs = lax.map(head_block, (normed.reshape(num_blocks, ROW_BLOCK, D), temperature.reshape(num_blocks, ROW_BLOCK), target.reshape(num_blocks, ROW_BLOCK)))
    return (log_norm.reshape(B), entropy.reshape(B), tgt_logp.reshape(B), logprobs.reshape(B, V))
```

```python
import functools

import jax
import jax.numpy as jnp
from jax import lax
from jax.experimental import pallas as pl
from jax.experimental.pallas import tpu as pltpu
from jax.sharding import PartitionSpec as P

NORM_EPS = 1e-6
ROWS = 128
LANES = 128
MESH = pl.DeviceIdType.MESH


class Sems:
    def __init__(self, ref):
        self.ref, self.used = ref, 0

    def take(self):
        self.used += 1
        return self.ref.at[self.used - 1]


def kernel(
    n2, n1,
    hidden, w_gate, w_up, w_down, gain, w_vocab, temp, target,
    out_ln, out_ent, out_tgt, out_lp,
    hid, wg, wu, wd, wv, acc_g, acc_u, act_t, yp, pair, chip, xr, ys, sq, xs,
    lg, far, mrg, dct, st2, st1,
    load_sems, send_sems, recv_sems,
):
    chunks, _, d_model = hid.shape
    ff_own = wg.shape[0]
    d_local = wd.shape[1]
    half = d_local // 2
    v_own = out_lp.shape[0]
    n_x = n1 // 2
    blk = ROWS // n_x
    y = lax.axis_index("tp2")
    tp = lax.axis_index("tp")
    x, core = tp // 2, tp % 2
    loads, sends, recvs = Sems(load_sems), Sems(send_sems), Sems(recv_sems)
    sent = []

    def at_y(j):
        return {"tp2": (y + j) % n2}

    def at_x(j):
        return {"tp": ((x + j) % n_x) * 2 + core}

    partner = {"tp": x * 2 + (1 - core)}

    def remote(src, dst, device):
        return pltpu.make_async_remote_copy(
            src_ref=src, dst_ref=dst, send_sem=sends.take(), recv_sem=recvs.take(),
            device_id=device, device_id_type=MESH,
        )

    def send(copy):
        copy.start()
        sent.append(copy)

    ff_cut = (ff_own // 2) // 16 * 16
    v_cut = (v_own // 2) // 8 * 8

    def act_rows(i, q, lo, size):
        return act_t.at[i, pl.ds(pl.multiple_of(q * ff_own + lo, 16), size), :]

    def q_of(slot):
        return (y + slot) % n2

    def base_of(slot):
        return pl.multiple_of((v_own * q_of(slot)) // 16 * 16, 16)

    def off_of(slot):
        return pl.multiple_of((v_own * q_of(slot)) % 16, 8)

    def lg_part(i, slot, part):
        lo, size = (0, v_cut) if part == 0 else (v_cut, v_own - v_cut)
        return lg.at[i, slot, pl.ds(pl.multiple_of(off_of(slot) + lo, 8), size), :]

    def part_of(buf, i, part):
        return buf.at[i, part, pl.ds(0, v_cut if part == 0 else v_own - v_cut), :]

    cps = []
    for i in range(chunks):
        c = {}
        own = act_rows(i, y, 0, ff_own)
        c["own_up"] = remote(own, own, at_y(1))
        c["own_dn"] = remote(own, own, at_y(-1))
        prev, nxt = (y + n2 - 1) % n2, (y + 1) % n2
        lo_half = act_rows(i, prev, 0, ff_cut)
        hi_half = act_rows(i, nxt, ff_cut, ff_own - ff_cut)
        c["fwd_up"] = remote(lo_half, lo_half, at_y(1))
        c["fwd_dn"] = remote(hi_half, hi_half, at_y(-1))
        c["pair"] = remote(yp.at[i, 1 - core], pair.at[i], partner)
        c["xrs"] = [
            remote(
                chip.at[i, pl.ds(pl.multiple_of(((x + j) % n_x) * blk, blk), blk), :],
                xr.at[i, j - 1], at_x(j),
            )
            for j in range(1, n_x)
        ]
        mine = ys.at[i, core, pl.ds(pl.multiple_of(x * blk, blk), blk), :]
        c["xag"] = [remote(mine, mine, at_x(j)) for j in range(1, n_x)]
        c["swap"] = remote(ys.at[i, core], ys.at[i, core], partner)
        c["ssq"] = [remote(sq.at[i, 0], sq.at[i, j], at_y(j)) for j in range(1, n2)]
        c["far_a"] = remote(lg_part(i, 2, 0), part_of(far, i, 0), at_y(-1))
        c["far_b"] = remote(lg_part(i, 2, 1), part_of(far, i, 1), at_y(1))
        c["dir_a"] = remote(lg_part(i, 1, 0), part_of(dct, i, 0), at_y(1))
        c["dir_b"] = remote(lg_part(i, 3, 1), part_of(dct, i, 1), at_y(-1))
        c["mrg_a"] = remote(lg_part(i, 3, 0), part_of(mrg, i, 0), at_y(-1))
        c["mrg_b"] = remote(lg_part(i, 1, 1), part_of(mrg, i, 1), at_y(1))
        c["st2"] = [remote(st2.at[i, 0], st2.at[i, j], at_y(j)) for j in range(1, n2)]
        c["st1"] = [
            remote(st1.at[i, 0], st1.at[i, j], {"tp": (tp + j) % n1}) for j in range(1, n1)
        ]
        cps.append(c)

    k_blocks = 4
    kb = d_model // k_blocks

    def load(src, dst):
        return pltpu.make_async_copy(src, dst, loads.take())

    ld_hid = [load(hidden.at[pl.ds(i * ROWS, ROWS), :], hid.at[i]) for i in range(chunks)]
    ld_w = [
        (
            load(w_gate.at[:, pl.ds(k * kb, kb)], wg.at[:, pl.ds(k * kb, kb)]),
            load(w_up.at[:, pl.ds(k * kb, kb)], wu.at[:, pl.ds(k * kb, kb)]),
        )
        for k in range(k_blocks)
    ]
    ld_wd = load(w_down, wd)
    ld_wv = load(w_vocab, wv)
    ld_hid[0].start()
    for pair_of in ld_w:
        for cp in pair_of:
            cp.start()
    for cp in ld_hid[1:]:
        cp.start()

    barrier = pltpu.get_barrier_semaphore()
    peers = [at_y(j) for j in range(1, n2)] + [{"tp": (tp + j) % n1} for j in range(1, n1)]
    for device in peers:
        pl.semaphore_signal(barrier, inc=1, device_id=device, device_id_type=MESH)
    pl.semaphore_wait(barrier, len(peers))

    NT = (((1,), (1,)), ((), ()))

    def gate_up(first, count):
        for i in range(first, first + count):
            ld_hid[i].wait()
        for k in range(k_blocks):
            cols = pl.ds(k * kb, kb)
            if first == 0:
                for cp in ld_w[k]:
                    cp.wait()
            h = hid[first:first + count, :, cols].reshape(count * ROWS, kb)
            g = lax.dot_general(wg[:, cols], h, NT, preferred_element_type=jnp.float32)
            u = lax.dot_general(wu[:, cols], h, NT, preferred_element_type=jnp.float32)
            if k == 0:
                acc_g[...] = g
                acc_u[...] = u
            else:
                acc_g[...] += g
                acc_u[...] += u
        act = (jax.nn.silu(acc_g[...]) * acc_u[...]).astype(jnp.bfloat16)
        for i in range(count):
            act_t[first + i, pl.ds(pl.multiple_of(y * ff_own, 16), ff_own), :] = (
                act[:, i * ROWS:(i + 1) * ROWS]
            )

    def send_own(i):
        send(cps[i]["own_up"])
        send(cps[i]["own_dn"])

    def forward(i):
        cps[i]["own_up"].wait_recv()
        send(cps[i]["fwd_up"])
        cps[i]["own_dn"].wait_recv()
        send(cps[i]["fwd_dn"])

    def down(i):
        cps[i]["fwd_up"].wait_recv()
        cps[i]["fwd_dn"].wait_recv()
        if i == 0:
            ld_wd.wait()
        for s in range(2):
            yp[i, s] = lax.dot_general(
                act_t[i], wd[:, s * half:(s + 1) * half],
                (((0,), (0,)), ((), ())), preferred_element_type=jnp.float32,
            ).astype(jnp.bfloat16)
        send(cps[i]["pair"])

    def chip_sum(i):
        cps[i]["pair"].wait_recv()
        chip[i] = (
            yp[i, core].astype(jnp.float32) + pair[i].astype(jnp.float32)
        ).astype(jnp.bfloat16)
        for cp in cps[i]["xrs"]:
            send(cp)

    def row_sum(i):
        at = pl.ds(pl.multiple_of(x * blk, blk), blk)
        total = chip[i, at, :].astype(jnp.float32)
        for j, cp in enumerate(cps[i]["xrs"]):
            cp.wait_recv()
            total += xr[i, j].astype(jnp.float32)
        ys[i, core, at, :] = total.astype(jnp.bfloat16)
        for cp in cps[i]["xag"]:
            send(cp)

    def swap(i):
        for cp in cps[i]["xag"]:
            cp.wait_recv()
        send(cps[i]["swap"])

    def residual(i, s):
        cols = pl.ds(pl.multiple_of(y * d_local + s * half, LANES), half)
        return hid[i, :, cols].astype(jnp.float32) + ys[i, s].astype(jnp.float32)

    def square(i):
        cps[i]["swap"].wait_recv()
        part = 0.0
        for s in range(2):
            r = residual(i, s)
            part = part + jnp.sum(r * r, axis=1, keepdims=True)
        sq[i, 0] = jnp.broadcast_to(part, (ROWS, LANES)).T[:8, :]
        for cp in cps[i]["ssq"]:
            send(cp)

    def norm(i):
        total = sq[i, 0]
        for j, cp in enumerate(cps[i]["ssq"]):
            cp.wait_recv()
            total = total + sq[i, j + 1]
        inv = lax.rsqrt(total / d_model + NORM_EPS)
        inv = jnp.broadcast_to(inv[:1, :], (LANES, ROWS)).T[:, :1]
        for s in range(2):
            g = gain[:, pl.ds(pl.multiple_of(y * d_local + s * half, LANES), half)]
            xs[i, :, s * half:(s + 1) * half] = (g * residual(i, s) * inv).astype(jnp.bfloat16)

    window = lg.shape[2]
    step = window // 3 if window % 48 == 0 else window

    def logits(i, slot):
        base = base_of(slot)

        @pl.loop(0, window // step)
        def _(j):
            at = pl.multiple_of(j * step, 16)
            lg[i, slot, pl.ds(at, step), :] = lax.dot_general(
                wv[pl.ds(pl.multiple_of(base + at, 16), step), :], xs[i], NT,
                preferred_element_type=jnp.float32,
            )

    def logits_far(i):
        logits(i, 2)
        send(cps[i]["far_a"])
        send(cps[i]["far_b"])

    def logits_near(i):
        logits(i, 1)
        send(cps[i]["dir_a"])
        logits(i, 3)
        send(cps[i]["dir_b"])

    def merge(i):
        for name, slot, part in (("a", 3, 0), ("b", 1, 1)):
            cps[i]["far_" + name].wait_recv()
            lg_part(i, slot, part)[...] += part_of(far, i, part)[...]
            send(cps[i]["mrg_" + name])

    def finish(i):
        logits(i, 0)
        lanes = pl.ds(i * ROWS, ROWS)
        t = temp[:, lanes]
        tgt = target[:, lanes]
        col0 = (tp * n2 + y) * v_own
        peak = None
        for part in range(2):
            cps[i]["dir_" + "ab"[part]].wait_recv()
            cps[i]["mrg_" + "ab"[part]].wait_recv()
            ref = lg_part(i, 0, part)
            val = (ref[...] + (part_of(dct, i, part)[...] + part_of(mrg, i, part)[...])) / t
            ref[...] = val
            top = jnp.max(val, axis=0, keepdims=True)
            peak = top if peak is None else jnp.maximum(peak, top)
        total = dot = hit = 0.0
        for part in range(2):
            val = lg_part(i, 0, part)[...]
            e = jnp.exp(val - peak)
            total = total + jnp.sum(e, axis=0, keepdims=True)
            dot = dot + jnp.sum(e * val, axis=0, keepdims=True)
            ids = col0 + part * v_cut + lax.broadcasted_iota(jnp.int32, val.shape, 0)
            hit = hit + jnp.sum(jnp.where(ids == tgt, val, 0.0), axis=0, keepdims=True)
        st2[i, 0, 0:1, :] = peak
        st2[i, 0, 1:2, :] = total
        st2[i, 0, 2:3, :] = dot
        st2[i, 0, 3:4, :] = hit
        st2[i, 0, 4:8, :] = jnp.zeros((4, ROWS), jnp.float32)
        for cp in cps[i]["st2"]:
            send(cp)

    def combine(tiles):
        peak = functools.reduce(jnp.maximum, [v[0:1, :] for v in tiles])
        total = dot = hit = 0.0
        for v in tiles:
            scale = jnp.exp(v[0:1, :] - peak)
            total = total + v[1:2, :] * scale
            dot = dot + v[2:3, :] * scale
            hit = hit + v[3:4, :]
        return peak, total, dot, hit

    def stats_y(i):
        for cp in cps[i]["st2"]:
            cp.wait_recv()
        vals = combine([st2[i, j] for j in range(n2)])
        for row, v in enumerate(vals):
            st1[i, 0, row:row + 1, :] = v
        st1[i, 0, 4:8, :] = jnp.zeros((4, ROWS), jnp.float32)
        for cp in cps[i]["st1"]:
            send(cp)

    def output(i):
        for cp in cps[i]["st1"]:
            cp.wait_recv()
        peak, total, dot, hit = combine([st1[i, j] for j in range(n1)])
        log_norm = peak + jnp.log(total)
        lanes = pl.ds(i * ROWS, ROWS)
        out_ln[:, lanes] = log_norm
        out_ent[:, lanes] = log_norm - dot / total
        out_tgt[:, lanes] = hit - log_norm
        val = lg[i, 0, pl.ds(off_of(0), v_own), :]
        out_lp[:, lanes] = (val - log_norm).astype(jnp.bfloat16)

    last = chunks - 1

    def run(*items):
        for fn, i in items:
            if 0 <= i <= last:
                fn(i)

    pack = acc_g.shape[1] // ROWS
    gate_up(0, pack)
    send_own(0)
    ld_wd.start()
    send_own(1)
    ld_wv.start()
    for i in range(pack, chunks, pack):
        gate_up(i, pack)
    run((forward, 0), (send_own, 2), (forward, 1), (send_own, 3))
    run((down, 0), (chip_sum, 0), (forward, 2), (down, 1), (row_sum, 0), (chip_sum, 1))
    run((forward, 3), (down, 2), (swap, 0), (row_sum, 1), (chip_sum, 2), (square, 0))
    run((down, 3), (swap, 1), (norm, 0))
    ld_wv.wait()
    run((logits_far, 0), (logits_near, 0))
    run((square, 1), (row_sum, 2), (chip_sum, 3), (norm, 1), (swap, 2), (row_sum, 3))
    run((square, 2), (swap, 3), (norm, 2), (square, 3), (norm, 3))
    for i in range(chunks):
        run((logits_far, i + 1), (merge, i), (logits_near, i + 1))
        run((finish, i - 1), (stats_y, i - 1), (output, i - 2))
    run((finish, last), (output, last - 1), (stats_y, last), (output, last))
    for cp in sent:
        cp.wait_send()


def solution(mesh):
    n2, n1 = mesh.shape["tp2"], mesh.shape["tp"]

    def device_step(hidden, w_gate, w_up, w_down, norm_gain, w_vocab, temperature, target):
        rows, d_model = hidden.shape
        ff_own = w_gate.shape[1]
        ff_tp, d_local = w_down.shape
        v_tp = w_vocab.shape[1]
        v_own = v_tp // n2
        chunks = rows // ROWS
        half = d_local // 2
        n_x = n1 // 2
        blk = ROWS // n_x
        pack = min(2, chunks)
        window = -(-v_own // 16) * 16
        part = v_own - (v_own // 2) // 8 * 8
        bf, f32 = jnp.bfloat16, jnp.float32
        n_loads = chunks + 8 + 2
        n_copies = chunks * (4 + 1 + (n_x - 1) * 2 + 1 + (n2 - 1) * 2 + 6 + n1 - 1)
        row = lambda a: a.reshape(1, -1)
        vmem = pl.BlockSpec(memory_space=pltpu.VMEM)
        hbm = pl.BlockSpec(memory_space=pl.ANY)
        ln, ent, tgt, lp = pl.pallas_call(
            functools.partial(kernel, n2, n1),
            out_shape=[
                jax.ShapeDtypeStruct((1, rows), f32),
                jax.ShapeDtypeStruct((1, rows), f32),
                jax.ShapeDtypeStruct((1, rows), f32),
                jax.ShapeDtypeStruct((v_own, rows), bf),
            ],
            in_specs=[hbm, hbm, hbm, hbm, vmem, hbm, vmem, vmem],
            out_specs=[vmem, vmem, vmem, vmem],
            scratch_shapes=[
                pltpu.VMEM((chunks, ROWS, d_model), bf),
                pltpu.VMEM((ff_own, d_model), bf),
                pltpu.VMEM((ff_own, d_model), bf),
                pltpu.VMEM((ff_tp, d_local), bf),
                pltpu.VMEM((v_tp, d_local), bf),
                pltpu.VMEM((ff_own, pack * ROWS), f32),
                pltpu.VMEM((ff_own, pack * ROWS), f32),
                pltpu.VMEM((chunks, ff_tp, ROWS), bf),
                pltpu.VMEM((chunks, 2, ROWS, half), bf),
                pltpu.VMEM((chunks, ROWS, half), bf),
                pltpu.VMEM((chunks, ROWS, half), bf),
                pltpu.VMEM((chunks, n_x - 1, blk, half), bf),
                pltpu.VMEM((chunks, 2, ROWS, half), bf),
                pltpu.VMEM((chunks, n2, 8, ROWS), f32),
                pltpu.VMEM((chunks, ROWS, d_local), bf),
                pltpu.VMEM((chunks, n2, window, ROWS), f32),
                pltpu.VMEM((chunks, 2, part, ROWS), f32),
                pltpu.VMEM((chunks, 2, part, ROWS), f32),
                pltpu.VMEM((chunks, 2, part, ROWS), f32),
                pltpu.VMEM((chunks, n2, 8, ROWS), f32),
                pltpu.VMEM((chunks, n1, 8, ROWS), f32),
                pltpu.SemaphoreType.DMA((n_loads,)),
                pltpu.SemaphoreType.DMA((n_copies,)),
                pltpu.SemaphoreType.DMA((n_copies,)),
            ],
            compiler_params=pltpu.CompilerParams(
                collective_id=0, has_side_effects=True, vmem_limit_bytes=66_000_000,
            ),
            name="decode_tail",
        )(
            hidden, w_gate.T, w_up.T, w_down, row(norm_gain), w_vocab.T,
            row(temperature), row(target),
        )
        return ln.reshape(rows), ent.reshape(rows), tgt.reshape(rows), lp.T

    return jax.shard_map(
        device_step, mesh=mesh,
        in_specs=(
            P("dp", None), P(None, ("tp", "tp2")), P(None, ("tp", "tp2")), P("tp", "tp2"),
            P(None), P("tp2", "tp"), P("dp"), P("dp"),
        ),
        out_specs=(P("dp"), P("dp"), P("dp"), P("dp", ("tp", "tp2"))),
        check_vma=False,
    )
```

```python
import functools

import jax
import jax.numpy as jnp
from jax import lax
from jax.experimental import pallas as pl
from jax.experimental.pallas import tpu as pltpu
from jax.sharding import PartitionSpec as P

NORM_EPS = 1e-6
ROWS = 128
LANES = 128
MESH = pl.DeviceIdType.MESH


class Sems:
    def __init__(self, ref):
        self.ref, self.used = ref, 0

    def take(self):
        self.used += 1
        return self.ref.at[self.used - 1]


def kernel(
    n2, n1,
    hidden, w_gate, w_up, w_down, gain_in, w_vocab, temp_in, target_in,
    out_row, out_lp,
    hid, wg, wu, wd, wv, acc_g, acc_u, act_t, yp, pair, chip, xr, ys, sq, xs,
    lg, far, mrg, dct, st2, st1, gain, temp, target, row_out, lp_out,
    load_sems, send_sems, recv_sems,
):
    chunks, _, d_model = hid.shape
    ff_own = wg.shape[0]
    d_local = wd.shape[1]
    half = d_local // 2
    v_own = out_lp.shape[0]
    n_x = n1 // 2
    blk = ROWS // n_x
    y = lax.axis_index("tp2")
    tp = lax.axis_index("tp")
    x, core = tp // 2, tp % 2
    loads, sends, recvs = Sems(load_sems), Sems(send_sems), Sems(recv_sems)
    sent = []

    def at_y(j):
        return {"tp2": (y + j) % n2}

    def at_x(j):
        return {"tp": ((x + j) % n_x) * 2 + core}

    partner = {"tp": x * 2 + (1 - core)}

    def remote(src, dst, device):
        return pltpu.make_async_remote_copy(
            src_ref=src, dst_ref=dst, send_sem=sends.take(), recv_sem=recvs.take(),
            device_id=device, device_id_type=MESH,
        )

    def send(copy):
        copy.start()
        sent.append(copy)

    ff_cut = (ff_own // 2) // 16 * 16
    v_cut = (v_own // 2) // 8 * 8

    def act_rows(i, q, lo, size):
        return act_t.at[i, pl.ds(pl.multiple_of(q * ff_own + lo, 16), size), :]

    def q_of(slot):
        return (y + slot) % n2

    def base_of(slot):
        return pl.multiple_of((v_own * q_of(slot)) // 16 * 16, 16)

    def off_of(slot):
        return pl.multiple_of((v_own * q_of(slot)) % 16, 8)

    def lg_part(i, slot, part):
        lo, size = (0, v_cut) if part == 0 else (v_cut, v_own - v_cut)
        return lg.at[i, slot, pl.ds(pl.multiple_of(off_of(slot) + lo, 8), size), :]

    def part_of(buf, i, part):
        return buf.at[i, part, pl.ds(0, v_cut if part == 0 else v_own - v_cut), :]

    cps = []
    for i in range(chunks):
        c = {}
        own = act_rows(i, y, 0, ff_own)
        c["own_up"] = remote(own, own, at_y(1))
        c["own_dn"] = remote(own, own, at_y(-1))
        prev, nxt = (y + n2 - 1) % n2, (y + 1) % n2
        lo_half = act_rows(i, prev, 0, ff_cut)
        hi_half = act_rows(i, nxt, ff_cut, ff_own - ff_cut)
        c["fwd_up"] = remote(lo_half, lo_half, at_y(1))
        c["fwd_dn"] = remote(hi_half, hi_half, at_y(-1))
        c["pair"] = remote(yp.at[i, 1 - core], pair.at[i], partner)
        c["xrs"] = [
            remote(
                chip.at[i, pl.ds(pl.multiple_of(((x + j) % n_x) * blk, blk), blk), :],
                xr.at[i, j - 1], at_x(j),
            )
            for j in range(1, n_x)
        ]
        mine = ys.at[i, core, pl.ds(pl.multiple_of(x * blk, blk), blk), :]
        c["xag"] = [remote(mine, mine, at_x(j)) for j in range(1, n_x)]
        c["swap"] = remote(ys.at[i, core], ys.at[i, core], partner)
        c["ssq"] = [remote(sq.at[i, 0], sq.at[i, j], at_y(j)) for j in range(1, n2)]
        c["far_a"] = remote(lg_part(i, 2, 0), part_of(far, i, 0), at_y(-1))
        c["far_b"] = remote(lg_part(i, 2, 1), part_of(far, i, 1), at_y(1))
        c["dir_a"] = remote(lg_part(i, 1, 0), part_of(dct, i, 0), at_y(1))
        c["dir_b"] = remote(lg_part(i, 3, 1), part_of(dct, i, 1), at_y(-1))
        c["mrg_a"] = remote(lg_part(i, 3, 0), part_of(mrg, i, 0), at_y(-1))
        c["mrg_b"] = remote(lg_part(i, 1, 1), part_of(mrg, i, 1), at_y(1))
        cps.append(c)
    cp_st2 = [remote(st2.at[0], st2.at[j], at_y(j)) for j in range(1, n2)]
    cp_st1 = [remote(st1.at[0], st1.at[j], {"tp": (tp + j) % n1}) for j in range(1, n1)]

    k_blocks = 5 if d_model % (5 * LANES) == 0 else 4
    kb = d_model // k_blocks

    def load(src, dst):
        return pltpu.make_async_copy(src, dst, loads.take())

    ld_hid = [load(hidden.at[pl.ds(i * ROWS, ROWS), :], hid.at[i]) for i in range(chunks)]
    ld_w = [
        (
            load(w_gate.at[:, pl.ds(k * kb, kb)], wg.at[:, pl.ds(k * kb, kb)]),
            load(w_up.at[:, pl.ds(k * kb, kb)], wu.at[:, pl.ds(k * kb, kb)]),
        )
        for k in range(k_blocks)
    ]
    ld_wd = load(w_down, wd)
    ld_wv = load(w_vocab, wv)
    ld_small = [load(gain_in, gain), load(temp_in, temp), load(target_in, target)]
    peers = [at_y(j) for j in range(1, n2)] + [{"tp": (tp + j) % n1} for j in range(1, n1)]
    with jax.named_scope("start"):
        ld_hid[0].start()
        for pair_of in ld_w[:1]:
            for cp in pair_of:
                cp.start()
        for cp in ld_hid[1:2]:
            cp.start()
        for pair_of in ld_w[1:]:
            for cp in pair_of:
                cp.start()
        for cp in ld_hid[2:] + ld_small:
            cp.start()
        barrier = pltpu.get_barrier_semaphore()
        for device in peers:
            pl.semaphore_signal(barrier, inc=1, device_id=device, device_id_type=MESH)

    NT = (((1,), (1,)), ((), ()))

    def gate_up(first, count):
        for i in range(first, first + count):
            ld_hid[i].wait()
        for k in range(k_blocks):
            cols = pl.ds(k * kb, kb)
            if first == 0:
                for cp in ld_w[k]:
                    cp.wait()
            h = hid[first:first + count, :, cols].reshape(count * ROWS, kb)
            g = lax.dot_general(wg[:, cols], h, NT, preferred_element_type=jnp.float32)
            u = lax.dot_general(wu[:, cols], h, NT, preferred_element_type=jnp.float32)
            if k == 0:
                acc_g[...] = g
                acc_u[...] = u
            else:
                acc_g[...] += g
                acc_u[...] += u
        act = (jax.nn.silu(acc_g[...]) * acc_u[...]).astype(jnp.bfloat16)
        for i in range(count):
            act_t[first + i, pl.ds(pl.multiple_of(y * ff_own, 16), ff_own), :] = (
                act[:, i * ROWS:(i + 1) * ROWS]
            )

    def send_own(i):
        send(cps[i]["own_up"])
        send(cps[i]["own_dn"])

    def forward(i):
        cps[i]["own_up"].wait_recv()
        send(cps[i]["fwd_up"])
        cps[i]["own_dn"].wait_recv()
        send(cps[i]["fwd_dn"])

    def down(i):
        cps[i]["fwd_up"].wait_recv()
        cps[i]["fwd_dn"].wait_recv()
        if i == 0:
            ld_wd.wait()
        for s in range(2):
            yp[i, s] = lax.dot_general(
                act_t[i], wd[:, s * half:(s + 1) * half],
                (((0,), (0,)), ((), ())), preferred_element_type=jnp.float32,
            ).astype(jnp.bfloat16)
        send(cps[i]["pair"])

    def chip_sum(i):
        cps[i]["pair"].wait_recv()
        chip[i] = (
            yp[i, core].astype(jnp.float32) + pair[i].astype(jnp.float32)
        ).astype(jnp.bfloat16)
        for cp in cps[i]["xrs"]:
            send(cp)

    def row_sum(i):
        at = pl.ds(pl.multiple_of(x * blk, blk), blk)
        total = chip[i, at, :].astype(jnp.float32)
        for j, cp in enumerate(cps[i]["xrs"]):
            cp.wait_recv()
            total += xr[i, j].astype(jnp.float32)
        ys[i, core, at, :] = total.astype(jnp.bfloat16)
        for cp in cps[i]["xag"]:
            send(cp)

    def swap(i):
        for cp in cps[i]["xag"]:
            cp.wait_recv()
        send(cps[i]["swap"])

    def residual(i, s):
        cols = pl.ds(pl.multiple_of(y * d_local + s * half, LANES), half)
        return hid[i, :, cols].astype(jnp.float32) + ys[i, s].astype(jnp.float32)

    def square(i):
        cps[i]["swap"].wait_recv()
        part = 0.0
        for s in range(2):
            r = residual(i, s)
            part = part + jnp.sum(r * r, axis=1, keepdims=True)
        sq[i, 0] = jnp.broadcast_to(part, (ROWS, LANES)).T[:8, :]
        for cp in cps[i]["ssq"]:
            send(cp)

    def norm(i):
        total = sq[i, 0]
        for j, cp in enumerate(cps[i]["ssq"]):
            cp.wait_recv()
            total = total + sq[i, j + 1]
        inv = lax.rsqrt(total / d_model + NORM_EPS)
        inv = jnp.broadcast_to(inv[:1, :], (LANES, ROWS)).T[:, :1]
        for s in range(2):
            g = gain[:, pl.ds(pl.multiple_of(y * d_local + s * half, LANES), half)]
            xs[i, :, s * half:(s + 1) * half] = (g * residual(i, s) * inv).astype(jnp.bfloat16)

    window = lg.shape[2]
    step = window // 3 if window % 48 == 0 else window

    def logits(i, slot):
        base = base_of(slot)

        @pl.loop(0, window // step)
        def _(j):
            at = pl.multiple_of(j * step, 16)
            lg[i, slot, pl.ds(at, step), :] = lax.dot_general(
                wv[pl.ds(pl.multiple_of(base + at, 16), step), :], xs[i], NT,
                preferred_element_type=jnp.float32,
            )

    def logits_far(i):
        logits(i, 2)
        send(cps[i]["far_a"])
        send(cps[i]["far_b"])

    def logits_near(i):
        logits(i, 1)
        send(cps[i]["dir_a"])
        logits(i, 3)
        send(cps[i]["dir_b"])

    def merge(i):
        for name, slot, part in (("a", 3, 0), ("b", 1, 1)):
            cps[i]["far_" + name].wait_recv()
            lg_part(i, slot, part)[...] += part_of(far, i, part)[...]
            send(cps[i]["mrg_" + name])

    def own(i):
        logits(i, 0)

    def near_sum(i):
        for part in range(2):
            cps[i]["dir_" + "ab"[part]].wait_recv()
            lg_part(i, 0, part)[...] += part_of(dct, i, part)[...]

    def finish(i):
        lanes = pl.ds(i * ROWS, ROWS)
        t = temp[:, lanes]
        tgt = target[:, lanes]
        col0 = (tp * n2 + y) * v_own
        peak = None
        for part in range(2):
            cps[i]["mrg_" + "ab"[part]].wait_recv()
            ref = lg_part(i, 0, part)
            val = (ref[...] + part_of(mrg, i, part)[...]) / t
            ref[...] = val
            top = jnp.max(val, axis=0, keepdims=True)
            peak = top if peak is None else jnp.maximum(peak, top)
        total = dot = hit = 0.0
        for part in range(2):
            val = lg_part(i, 0, part)[...]
            e = jnp.exp(val - peak)
            total = total + jnp.sum(e, axis=0, keepdims=True)
            dot = dot + jnp.sum(e * val, axis=0, keepdims=True)
            ids = col0 + part * v_cut + lax.broadcasted_iota(jnp.int32, val.shape, 0)
            hit = hit + jnp.sum(jnp.where(ids == tgt, val, 0.0), axis=0, keepdims=True)
        for row, v in enumerate((peak, total, dot, hit)):
            st2[0, row, :, lanes] = v

    def combine(tiles):
        peak = functools.reduce(jnp.maximum, [v[0] for v in tiles])
        total = dot = hit = 0.0
        for v in tiles:
            scale = jnp.exp(v[0] - peak)
            total = total + v[1] * scale
            dot = dot + v[2] * scale
            hit = hit + v[3]
        return peak, total, dot, hit

    def stats_y():
        for cp in cp_st2:
            send(cp)
        for cp in cp_st2:
            cp.wait_recv()
        for row, v in enumerate(combine([st2[j] for j in range(n2)])):
            st1[0, row] = v
        for cp in cp_st1:
            send(cp)

    def output():
        for cp in cp_st1:
            cp.wait_recv()
        peak, total, dot, hit = combine([st1[j] for j in range(n1)])
        log_norm = peak + jnp.log(total)
        row_out[0:1, :] = log_norm
        row_out[1:2, :] = log_norm - dot / total
        row_out[2:3, :] = hit - log_norm
        for i in range(chunks):
            lanes = slice(i * ROWS, (i + 1) * ROWS)
            val = lg[i, 0, pl.ds(off_of(0), v_own), :]
            lp_out[:, lanes] = (val - log_norm[:, lanes]).astype(jnp.bfloat16)

    last = chunks - 1

    def run(*items):
        for fn, i in items:
            if 0 <= i <= last:
                with jax.named_scope(f"{fn.__name__}#c={i}"):
                    fn(i)

    def produce(i):
        gate_up(i, pack)

    pack = acc_g.shape[1] // ROWS
    run((produce, 0))
    with jax.named_scope("barrier"):
        pl.semaphore_wait(barrier, len(peers))
    run((send_own, 0))
    ld_wd.start()
    run((send_own, 1))
    ld_wv.start()
    for i in range(pack, chunks, pack):
        run((produce, i))
    for cp in ld_small:
        cp.wait()
    run((forward, 0), (send_own, 2), (forward, 1), (send_own, 3))
    run((down, 0), (chip_sum, 0), (down, 1), (forward, 2), (chip_sum, 1), (row_sum, 0))
    run((forward, 3), (down, 2), (row_sum, 1), (chip_sum, 2), (swap, 0), (down, 3))
    run((square, 0), (chip_sum, 3), (row_sum, 2), (swap, 1), (norm, 0), (square, 1))
    ld_wv.wait()
    run((logits_far, 0), (swap, 2), (row_sum, 3), (square, 2), (norm, 1), (logits_near, 0))
    run((swap, 3), (square, 3), (logits_far, 1), (norm, 2), (merge, 0), (logits_near, 1), (norm, 3))
    for i in range(1, chunks - 1):
        run((logits_far, i + 1), (merge, i), (logits_near, i + 1))
        run((own, i - 1), (near_sum, i - 1))
    run((finish, last - 3), (own, last - 1), (own, last), (near_sum, last - 1), (finish, last - 2))
    run((merge, last), (finish, last - 1), (near_sum, last), (finish, last))
    with jax.named_scope("stats_y"):
        stats_y()
    with jax.named_scope("output"):
        output()
    with jax.named_scope("drain"):
        stores = [load(row_out, out_row), load(lp_out, out_lp)]
        for cp in stores:
            cp.start()
        for cp in sent:
            cp.wait_send()
        for cp in stores:
            cp.wait()


def emit(rows_in, lp_in, ln, ent, tgt, lp):
    ln[...] = rows_in[0:1, :]
    ent[...] = rows_in[1:2, :]
    tgt[...] = rows_in[2:3, :]
    lp[...] = lp_in[...]


def solution(mesh):
    n2, n1 = mesh.shape["tp2"], mesh.shape["tp"]

    def device_step(hidden, w_gate, w_up, w_down, norm_gain, w_vocab, temperature, target):
        rows, d_model = hidden.shape
        ff_own = w_gate.shape[1]
        ff_tp, d_local = w_down.shape
        v_tp = w_vocab.shape[1]
        v_own = v_tp // n2
        chunks = rows // ROWS
        half = d_local // 2
        n_x = n1 // 2
        blk = ROWS // n_x
        pack = min(2, chunks)
        window = -(-v_own // 16) * 16
        part = v_own - (v_own // 2) // 8 * 8
        bf, f32 = jnp.bfloat16, jnp.float32
        n_loads = chunks + 10 + 2 + 3 + 2
        n_copies = chunks * (4 + 1 + (n_x - 1) * 2 + 1 + n2 - 1 + 6) + n2 - 1 + n1 - 1
        row = lambda a: a.reshape(1, -1)
        vmem = pl.BlockSpec(memory_space=pltpu.VMEM)
        hbm = pl.BlockSpec(memory_space=pl.ANY)
        results = [
            jax.ShapeDtypeStruct((1, rows), f32),
            jax.ShapeDtypeStruct((1, rows), f32),
            jax.ShapeDtypeStruct((1, rows), f32),
            jax.ShapeDtypeStruct((v_own, rows), bf),
        ]
        parts = pl.pallas_call(
            functools.partial(kernel, n2, n1),
            out_shape=[jax.ShapeDtypeStruct((8, rows), f32), results[3]],
            in_specs=[hbm] * 8,
            out_specs=[hbm, hbm],
            scratch_shapes=[
                pltpu.VMEM((chunks, ROWS, d_model), bf),
                pltpu.VMEM((ff_own, d_model), bf),
                pltpu.VMEM((ff_own, d_model), bf),
                pltpu.VMEM((ff_tp, d_local), bf),
                pltpu.VMEM((v_tp, d_local), bf),
                pltpu.VMEM((ff_own, pack * ROWS), f32),
                pltpu.VMEM((ff_own, pack * ROWS), f32),
                pltpu.VMEM((chunks, ff_tp, ROWS), bf),
                pltpu.VMEM((chunks, 2, ROWS, half), bf),
                pltpu.VMEM((chunks, ROWS, half), bf),
                pltpu.VMEM((chunks, ROWS, half), bf),
                pltpu.VMEM((chunks, n_x - 1, blk, half), bf),
                pltpu.VMEM((chunks, 2, ROWS, half), bf),
                pltpu.VMEM((chunks, n2, 8, ROWS), f32),
                pltpu.VMEM((chunks, ROWS, d_local), bf),
                pltpu.VMEM((chunks, n2, window, ROWS), f32),
                pltpu.VMEM((chunks, 2, part, ROWS), f32),
                pltpu.VMEM((chunks, 2, part, ROWS), f32),
                pltpu.VMEM((chunks, 2, part, ROWS), f32),
                pltpu.VMEM((n2, 4, 1, rows), f32),
                pltpu.VMEM((n1, 4, 1, rows), f32),
                pltpu.VMEM((1, d_model), f32),
                pltpu.VMEM((1, rows), f32),
                pltpu.VMEM((1, rows), jnp.int32),
                pltpu.VMEM((8, rows), f32),
                pltpu.VMEM((v_own, rows), bf),
                pltpu.SemaphoreType.DMA((n_loads,)),
                pltpu.SemaphoreType.DMA((n_copies,)),
                pltpu.SemaphoreType.DMA((n_copies,)),
            ],
            compiler_params=pltpu.CompilerParams(
                collective_id=0, has_side_effects=True, vmem_limit_bytes=66_000_000,
            ),
            name="decode_tail",
        )(
            hidden, w_gate.T, w_up.T, w_down, row(norm_gain), w_vocab.T,
            row(temperature), row(target),
        )
        ln, ent, tgt, lp = pl.pallas_call(
            emit, out_shape=results, in_specs=[vmem] * 2, out_specs=[vmem] * 4, name="emit",
        )(*parts)
        return ln.reshape(rows), ent.reshape(rows), tgt.reshape(rows), lp.T

    return jax.shard_map(
        device_step, mesh=mesh,
        in_specs=(
            P("dp", None), P(None, ("tp", "tp2")), P(None, ("tp", "tp2")), P("tp", "tp2"),
            P(None), P("tp2", "tp"), P("dp"), P("dp"),
        ),
        out_specs=(P("dp"), P("dp"), P("dp"), P("dp", ("tp", "tp2"))),
        check_vma=False,
    )
```

```python
import functools

import jax
import jax.numpy as jnp
from jax import lax
from jax.experimental import pallas as pl
from jax.experimental.pallas import tpu as pltpu
from jax.sharding import PartitionSpec as P

NORM_EPS = 1e-6
ROWS = 128
LANES = 128
MESH = pl.DeviceIdType.MESH


class Sems:
    def __init__(self, ref):
        self.ref, self.used = ref, 0

    def take(self):
        self.used += 1
        return self.ref.at[self.used - 1]


def kernel(
    n2, n1,
    hidden, w_gate, w_up, w_down, gain_in, w_vocab, temp_in, target_in,
    out_row, out_lp,
    hid, wg, wu, wd, wv, acc_g, acc_u, act_t, yp, pair, chip, xr, ys, sq, xs,
    lg, far, mrg, dct, sq_col, sq_all, st_a, st_b, gain, temp, target, row_out, lp_out,
    load_sems, send_sems, recv_sems, cast_sems,
):
    chunks, _, d_model = hid.shape
    ff_own = wg.shape[0]
    d_local = wd.shape[1]
    half = d_local // 2
    v_own = out_lp.shape[0]
    n_x = n1 // 2
    blk = ROWS // n_x
    y = lax.axis_index("tp2")
    tp = lax.axis_index("tp")
    x, core = tp // 2, tp % 2
    loads, sends, recvs = Sems(load_sems), Sems(send_sems), Sems(recv_sems)
    sent = []

    def at_y(j):
        return {"tp2": (y + j) % n2}

    def at_x(j):
        return {"tp": ((x + j) % n_x) * 2 + core}

    partner = {"tp": x * 2 + (1 - core)}

    def remote(src, dst, device):
        return pltpu.make_async_remote_copy(
            src_ref=src, dst_ref=dst, send_sem=sends.take(), recv_sem=recvs.take(),
            device_id=device, device_id_type=MESH,
        )

    def send(copy):
        copy.start()
        sent.append(copy)

    everyone = [(j2, j1) for j2 in range(n2) for j1 in range(n1)][1:]
    casts = []

    def slot_of(y_from, tp_from):
        return ((y + n2 - y_from) % n2) * n1 + (tp + n1 - tp_from) % n1

    def broadcast(buf, index):
        for j2, j1 in everyone:
            pltpu.make_async_remote_copy(
                src_ref=buf.at[0], dst_ref=buf.at[j2 * n1 + j1],
                send_sem=cast_sems.at[index, 0], recv_sem=cast_sems.at[index, 1],
                device_id={"tp2": (y + j2) % n2, "tp": (tp + j1) % n1}, device_id_type=MESH,
            ).start()
        casts.append((buf, index))

    def wait_cast(buf, index, side):
        rest = buf.at[pl.ds(1, n2 * n1 - 1)]
        pltpu.make_async_copy(rest, rest, cast_sems.at[index, side]).wait()

    ff_cut = (ff_own // 2) // 16 * 16
    v_cut = (v_own // 2) // 8 * 8

    def act_rows(i, q, lo, size):
        return act_t.at[i, pl.ds(pl.multiple_of(q * ff_own + lo, 16), size), :]

    def q_of(slot):
        return (y + slot) % n2

    def base_of(slot):
        return pl.multiple_of((v_own * q_of(slot)) // 16 * 16, 16)

    def off_of(slot):
        return pl.multiple_of((v_own * q_of(slot)) % 16, 8)

    def lg_part(i, slot, part):
        lo, size = (0, v_cut) if part == 0 else (v_cut, v_own - v_cut)
        return lg.at[i, slot, pl.ds(pl.multiple_of(off_of(slot) + lo, 8), size), :]

    def part_of(buf, i, part):
        return buf.at[i, part, pl.ds(0, v_cut if part == 0 else v_own - v_cut), :]

    cps = []
    for i in range(chunks):
        c = {}
        own = act_rows(i, y, 0, ff_own)
        c["own_up"] = remote(own, own, at_y(1))
        c["own_dn"] = remote(own, own, at_y(-1))
        prev, nxt = (y + n2 - 1) % n2, (y + 1) % n2
        lo_half = act_rows(i, prev, 0, ff_cut)
        hi_half = act_rows(i, nxt, ff_cut, ff_own - ff_cut)
        if i == 0:
            lo_half = act_rows(i, y, 0, ff_cut)
            hi_half = act_rows(i, y, ff_cut, ff_own - ff_cut)
            c["fwd_up"] = remote(lo_half, lo_half, at_y(2))
            c["fwd_dn"] = remote(hi_half, hi_half, at_y(-2))
        else:
            c["fwd_up"] = remote(lo_half, lo_half, at_y(1))
            c["fwd_dn"] = remote(hi_half, hi_half, at_y(-1))
        c["pair"] = remote(yp.at[i, 1 - core], pair.at[i], partner)
        c["xrs"] = [
            remote(
                chip.at[i, pl.ds(pl.multiple_of(((x + j) % n_x) * blk, blk), blk), :],
                xr.at[i, j - 1], at_x(j),
            )
            for j in range(1, n_x)
        ]
        mine = ys.at[i, core, pl.ds(pl.multiple_of(x * blk, blk), blk), :]
        c["xag"] = [remote(mine, mine, at_x(j)) for j in range(1, n_x)]
        c["swap"] = remote(ys.at[i, core], ys.at[i, core], partner)
        c["ssq"] = [] if i == 0 else [remote(sq.at[i, 0], sq.at[i, j], at_y(j)) for j in range(1, n2)]
        c["far_a"] = remote(lg_part(i, 2, 0), part_of(far, i, 0), at_y(-1))
        c["far_b"] = remote(lg_part(i, 2, 1), part_of(far, i, 1), at_y(1))
        c["dir_a"] = remote(lg_part(i, 1, 0), part_of(dct, i, 0), at_y(1))
        c["dir_b"] = remote(lg_part(i, 3, 1), part_of(dct, i, 1), at_y(-1))
        c["mrg_a"] = remote(lg_part(i, 3, 0), part_of(mrg, i, 0), at_y(-1))
        c["mrg_b"] = remote(lg_part(i, 1, 1), part_of(mrg, i, 1), at_y(1))
        cps.append(c)

    k_blocks = 5 if d_model % (5 * LANES) == 0 else 4
    kb = d_model // k_blocks

    def load(src, dst):
        return pltpu.make_async_copy(src, dst, loads.take())

    ld_hid = [load(hidden.at[pl.ds(i * ROWS, ROWS), :], hid.at[i]) for i in range(chunks)]
    ld_w = [
        (
            load(w_gate.at[:, pl.ds(k * kb, kb)], wg.at[:, pl.ds(k * kb, kb)]),
            load(w_up.at[:, pl.ds(k * kb, kb)], wu.at[:, pl.ds(k * kb, kb)]),
        )
        for k in range(k_blocks)
    ]
    ld_wd = load(w_down, wd)
    ld_wv = load(w_vocab, wv)
    ld_small = [load(gain_in, gain), load(temp_in, temp), load(target_in, target)]
    peers = [{"tp2": (y + j2) % n2, "tp": (tp + j1) % n1} for j2, j1 in everyone]
    with jax.named_scope("start"):
        ld_hid[0].start()
        for pair_of in ld_w[:1]:
            for cp in pair_of:
                cp.start()
        for cp in ld_hid[1:2]:
            cp.start()
        for pair_of in ld_w[1:]:
            for cp in pair_of:
                cp.start()
        for cp in ld_small:
            cp.start()
        barrier = pltpu.get_barrier_semaphore()
        for device in peers:
            pl.semaphore_signal(barrier, inc=1, device_id=device, device_id_type=MESH)

    NT = (((1,), (1,)), ((), ()))

    def gate_up(first, count):
        for i in range(first, first + count):
            ld_hid[i].wait()
        for k in range(k_blocks):
            cols = pl.ds(k * kb, kb)
            if first == 0 and k == k_blocks - 1:
                for cp in ld_hid[2:]:
                    cp.start()
            if first == 0:
                for cp in ld_w[k]:
                    cp.wait()
            h = hid[first:first + count, :, cols].reshape(count * ROWS, kb)
            g = lax.dot_general(wg[:, cols], h, NT, preferred_element_type=jnp.float32)
            u = lax.dot_general(wu[:, cols], h, NT, preferred_element_type=jnp.float32)
            if k == 0:
                acc_g[...] = g
                acc_u[...] = u
            else:
                acc_g[...] += g
                acc_u[...] += u
        act = (jax.nn.silu(acc_g[...]) * acc_u[...]).astype(jnp.bfloat16)
        for i in range(count):
            act_t[first + i, pl.ds(pl.multiple_of(y * ff_own, 16), ff_own), :] = (
                act[:, i * ROWS:(i + 1) * ROWS]
            )

    def send_own(i):
        send(cps[i]["own_up"])
        send(cps[i]["own_dn"])
        if i == 0:
            send(cps[i]["fwd_up"])
            send(cps[i]["fwd_dn"])

    def forward(i):
        cps[i]["own_up"].wait_recv()
        send(cps[i]["fwd_up"])
        cps[i]["own_dn"].wait_recv()
        send(cps[i]["fwd_dn"])

    def down(i):
        if i == 0:
            cps[i]["own_up"].wait_recv()
            cps[i]["own_dn"].wait_recv()
        cps[i]["fwd_up"].wait_recv()
        cps[i]["fwd_dn"].wait_recv()
        if i == 0:
            ld_wd.wait()
        for s in range(2):
            yp[i, s] = lax.dot_general(
                act_t[i], wd[:, s * half:(s + 1) * half],
                (((0,), (0,)), ((), ())), preferred_element_type=jnp.float32,
            ).astype(jnp.bfloat16)
        send(cps[i]["pair"])

    def chip_sum(i):
        cps[i]["pair"].wait_recv()
        chip[i] = (
            yp[i, core].astype(jnp.float32) + pair[i].astype(jnp.float32)
        ).astype(jnp.bfloat16)
        for cp in cps[i]["xrs"]:
            send(cp)

    def row_sum(i):
        at = pl.ds(pl.multiple_of(x * blk, blk), blk)
        total = chip[i, at, :].astype(jnp.float32)
        for j, cp in enumerate(cps[i]["xrs"]):
            cp.wait_recv()
            total += xr[i, j].astype(jnp.float32)
        total = total.astype(jnp.bfloat16)
        ys[i, core, at, :] = total
        for cp in cps[i]["xag"]:
            send(cp)
        if i == 0:
            cols = pl.ds(pl.multiple_of(y * d_local + core * half, LANES), half)
            r = hid[i, at, cols].astype(jnp.float32) + total.astype(jnp.float32)
            part = jnp.sum(r * r, axis=1, keepdims=True)
            sq_col[...] = jnp.zeros_like(sq_col)
            sq_col[at, :] = jnp.broadcast_to(part, (blk, LANES))
            sq_all[0] = sq_col[...].T[:8, :]
            broadcast(sq_all, 0)

    def swap(i):
        for cp in cps[i]["xag"]:
            cp.wait_recv()
        send(cps[i]["swap"])

    def residual(i, s):
        cols = pl.ds(pl.multiple_of(y * d_local + s * half, LANES), half)
        return hid[i, :, cols].astype(jnp.float32) + ys[i, s].astype(jnp.float32)

    def square(i):
        cps[i]["swap"].wait_recv()
        part = 0.0
        for s in range(2):
            r = residual(i, s)
            part = part + jnp.sum(r * r, axis=1, keepdims=True)
        sq[i, 0] = jnp.broadcast_to(part, (ROWS, LANES)).T[:8, :]
        for cp in cps[i]["ssq"]:
            send(cp)

    def norm(i):
        if i == 0:
            cps[i]["swap"].wait_recv()
            wait_cast(sq_all, 0, 1)
            total = jnp.sum(sq_all[...], axis=0)
        else:
            total = sq[i, 0]
            for j, cp in enumerate(cps[i]["ssq"]):
                cp.wait_recv()
                total = total + sq[i, j + 1]
        inv = lax.rsqrt(total / d_model + NORM_EPS)
        inv = jnp.broadcast_to(inv[:1, :], (LANES, ROWS)).T[:, :1]
        for s in range(2):
            g = gain[:, pl.ds(pl.multiple_of(y * d_local + s * half, LANES), half)]
            xs[i, :, s * half:(s + 1) * half] = (g * residual(i, s) * inv).astype(jnp.bfloat16)

    window = lg.shape[2]
    step = window // 3 if window % 48 == 0 else window

    def logits(i, slot):
        base = base_of(slot)

        @pl.loop(0, window // step)
        def _(j):
            at = pl.multiple_of(j * step, 16)
            lg[i, slot, pl.ds(at, step), :] = lax.dot_general(
                wv[pl.ds(pl.multiple_of(base + at, 16), step), :], xs[i], NT,
                preferred_element_type=jnp.float32,
            )

    def logits_far(i):
        logits(i, 2)
        send(cps[i]["far_a"])
        send(cps[i]["far_b"])

    def logits_near(i):
        logits(i, 1)
        if i > 0:
            send(cps[i]["dir_a"])
        logits(i, 3)
        if i > 0:
            send(cps[i]["dir_b"])

    def near_send(i):
        send(cps[i]["dir_a"])
        send(cps[i]["dir_b"])

    def merge(i):
        for name, slot, part in (("a", 3, 0), ("b", 1, 1)):
            cps[i]["far_" + name].wait_recv()
            lg_part(i, slot, part)[...] += part_of(far, i, part)[...]
            send(cps[i]["mrg_" + name])

    def own(i):
        logits(i, 0)

    def near_sum(i):
        for part in range(2):
            cps[i]["dir_" + "ab"[part]].wait_recv()
            lg_part(i, 0, part)[...] += part_of(dct, i, part)[...]

    def finish(i):
        lanes = pl.ds(i * ROWS, ROWS)
        t = temp[:, lanes]
        tgt = target[:, lanes]
        col0 = (tp * n2 + y) * v_own
        peak = None
        for part in range(2):
            cps[i]["mrg_" + "ab"[part]].wait_recv()
            ref = lg_part(i, 0, part)
            val = (ref[...] + part_of(mrg, i, part)[...]) / t
            ref[...] = val
            top = jnp.max(val, axis=0, keepdims=True)
            peak = top if peak is None else jnp.maximum(peak, top)
        total = dot = hit = 0.0
        for part in range(2):
            val = lg_part(i, 0, part)[...]
            e = jnp.exp(val - peak)
            total = total + jnp.sum(e, axis=0, keepdims=True)
            dot = dot + jnp.sum(e * val, axis=0, keepdims=True)
            ids = col0 + part * v_cut + lax.broadcasted_iota(jnp.int32, val.shape, 0)
            hit = hit + jnp.sum(jnp.where(ids == tgt, val, 0.0), axis=0, keepdims=True)
        buf, at = (st_b, slice(0, ROWS)) if i == chunks - 1 else (st_a, lanes)
        for row, v in enumerate((peak, total, dot, hit)):
            buf[0, row, :, at] = v

    def combine(buf, lanes):
        peak = jnp.max(buf[:, 0], axis=0)
        total = dot = hit = 0.0
        for j2 in range(n2):
            for j1 in range(n1):
                v = buf[slot_of(j2, j1)]
                scale = jnp.exp(v[0] - peak)
                total = total + v[1] * scale
                dot = dot + v[2] * scale
                hit = hit + v[3]
        log_norm = peak + jnp.log(total)
        row_out[0:1, lanes] = log_norm
        row_out[1:2, lanes] = log_norm - dot / total
        row_out[2:3, lanes] = hit - log_norm

    def output(first, count):
        for i in range(first, first + count):
            lanes = slice(i * ROWS, (i + 1) * ROWS)
            val = lg[i, 0, pl.ds(off_of(0), v_own), :]
            lp_out[:, lanes] = (val - row_out[0:1, lanes]).astype(jnp.bfloat16)

    last = chunks - 1

    def run(*items):
        for fn, i in items:
            if 0 <= i <= last:
                with jax.named_scope(f"{fn.__name__}#c={i}"):
                    fn(i)

    def produce(i):
        gate_up(i, pack)

    pack = acc_g.shape[1] // ROWS
    run((produce, 0))
    with jax.named_scope("barrier"):
        pl.semaphore_wait(barrier, len(peers))
    run((send_own, 0))
    ld_wd.start()
    run((send_own, 1))
    ld_wv.start()
    for i in range(pack, chunks, pack):
        run((produce, i))
    for cp in ld_small:
        cp.wait()
    run((send_own, 2), (down, 0), (chip_sum, 0), (forward, 1), (send_own, 3), (row_sum, 0))
    run((forward, 2), (down, 1), (swap, 0), (forward, 3), (chip_sum, 1), (norm, 0))
    ld_wv.wait()
    run((logits_far, 0), (row_sum, 1), (down, 2), (logits_near, 0), (chip_sum, 2), (swap, 1))
    run((down, 3), (square, 1), (near_send, 0), (row_sum, 2), (chip_sum, 3), (swap, 2), (row_sum, 3))
    run((square, 2), (norm, 1), (logits_far, 1), (swap, 3), (square, 3), (merge, 0), (logits_near, 1))
    run((norm, 2),)
    for i in range(1, chunks - 1):
        run((logits_far, i + 1), (merge, i), (logits_near, i + 1), (norm, i + 2))
        run((own, i - 1), (near_sum, i - 1))
    run((finish, last - 3), (own, last - 1), (own, last), (near_sum, last - 1), (finish, last - 2))
    run((merge, last), (finish, last - 1))
    with jax.named_scope("cast_a"):
        broadcast(st_a, 1)
    run((near_sum, last), (finish, last))
    with jax.named_scope("cast_b"):
        broadcast(st_b, 2)
    with jax.named_scope("output_a"):
        wait_cast(st_a, 1, 1)
        combine(st_a, slice(0, last * ROWS))
        output(0, last)
        first_store = load(lp_out.at[:, :last * ROWS], out_lp.at[:, :last * ROWS])
        first_store.start()
    with jax.named_scope("sent"):
        for cp in sent:
            cp.wait_send()
    with jax.named_scope("wait_b"):
        wait_cast(st_b, 2, 1)
    with jax.named_scope("output_b"):
        combine(st_b, slice(last * ROWS, chunks * ROWS))
        output(last, 1)
    with jax.named_scope("drain"):
        stores = [load(row_out, out_row), load(lp_out.at[:, last * ROWS:], out_lp.at[:, last * ROWS:])]
        for cp in stores:
            cp.start()
        for buf, index in casts:
            wait_cast(buf, index, 0)
        for cp in [first_store] + stores:
            cp.wait()


def emit(rows_in, lp_in, ln, ent, tgt, lp):
    ln[...] = rows_in[0:1, :]
    ent[...] = rows_in[1:2, :]
    tgt[...] = rows_in[2:3, :]
    lp[...] = lp_in[...]


def solution(mesh):
    n2, n1 = mesh.shape["tp2"], mesh.shape["tp"]

    def device_step(hidden, w_gate, w_up, w_down, norm_gain, w_vocab, temperature, target):
        rows, d_model = hidden.shape
        ff_own = w_gate.shape[1]
        ff_tp, d_local = w_down.shape
        v_tp = w_vocab.shape[1]
        v_own = v_tp // n2
        chunks = rows // ROWS
        half = d_local // 2
        n_x = n1 // 2
        blk = ROWS // n_x
        pack = min(2, chunks)
        window = -(-v_own // 16) * 16
        part = v_own - (v_own // 2) // 8 * 8
        bf, f32 = jnp.bfloat16, jnp.float32
        n_loads = chunks + 10 + 2 + 3 + 3
        n_copies = chunks * (4 + 1 + (n_x - 1) * 2 + 1 + 6) + (chunks - 1) * (n2 - 1)
        row = lambda a: a.reshape(1, -1)
        vmem = pl.BlockSpec(memory_space=pltpu.VMEM)
        hbm = pl.BlockSpec(memory_space=pl.ANY)
        results = [
            jax.ShapeDtypeStruct((1, rows), f32),
            jax.ShapeDtypeStruct((1, rows), f32),
            jax.ShapeDtypeStruct((1, rows), f32),
            jax.ShapeDtypeStruct((v_own, rows), bf),
        ]
        parts = pl.pallas_call(
            functools.partial(kernel, n2, n1),
            out_shape=[jax.ShapeDtypeStruct((8, rows), f32), results[3]],
            in_specs=[hbm] * 8,
            out_specs=[hbm, hbm],
            scratch_shapes=[
                pltpu.VMEM((chunks, ROWS, d_model), bf),
                pltpu.VMEM((ff_own, d_model), bf),
                pltpu.VMEM((ff_own, d_model), bf),
                pltpu.VMEM((ff_tp, d_local), bf),
                pltpu.VMEM((v_tp, d_local), bf),
                pltpu.VMEM((ff_own, pack * ROWS), f32),
                pltpu.VMEM((ff_own, pack * ROWS), f32),
                pltpu.VMEM((chunks, ff_tp, ROWS), bf),
                pltpu.VMEM((chunks, 2, ROWS, half), bf),
                pltpu.VMEM((chunks, ROWS, half), bf),
                pltpu.VMEM((chunks, ROWS, half), bf),
                pltpu.VMEM((chunks, n_x - 1, blk, half), bf),
                pltpu.VMEM((chunks, 2, ROWS, half), bf),
                pltpu.VMEM((chunks, n2, 8, ROWS), f32),
                pltpu.VMEM((chunks, ROWS, d_local), bf),
                pltpu.VMEM((chunks, n2, window, ROWS), f32),
                pltpu.VMEM((chunks, 2, part, ROWS), f32),
                pltpu.VMEM((chunks, 2, part, ROWS), f32),
                pltpu.VMEM((chunks, 2, part, ROWS), f32),
                pltpu.VMEM((ROWS, LANES), f32),
                pltpu.VMEM((n2 * n1, 8, ROWS), f32),
                pltpu.VMEM((n2 * n1, 4, 1, rows - ROWS), f32),
                pltpu.VMEM((n2 * n1, 4, 1, ROWS), f32),
                pltpu.VMEM((1, d_model), f32),
                pltpu.VMEM((1, rows), f32),
                pltpu.VMEM((1, rows), jnp.int32),
                pltpu.VMEM((8, rows), f32),
                pltpu.VMEM((v_own, rows), bf),
                pltpu.SemaphoreType.DMA((n_loads,)),
                pltpu.SemaphoreType.DMA((n_copies,)),
                pltpu.SemaphoreType.DMA((n_copies,)),
                pltpu.SemaphoreType.DMA((3, 2)),
            ],
            compiler_params=pltpu.CompilerParams(
                collective_id=0, has_side_effects=True, vmem_limit_bytes=66_000_000,
            ),
            name="decode_tail",
        )(
            hidden, w_gate.T, w_up.T, w_down, row(norm_gain), w_vocab.T,
            row(temperature), row(target),
        )
        ln, ent, tgt, lp = pl.pallas_call(
            emit, out_shape=results, in_specs=[vmem] * 2, out_specs=[vmem] * 4, name="emit",
        )(*parts)
        return ln.reshape(rows), ent.reshape(rows), tgt.reshape(rows), lp.T

    return jax.shard_map(
        device_step, mesh=mesh,
        in_specs=(
            P("dp", None), P(None, ("tp", "tp2")), P(None, ("tp", "tp2")), P("tp", "tp2"),
            P(None), P("tp2", "tp"), P("dp"), P("dp"),
        ),
        out_specs=(P("dp"), P("dp"), P("dp"), P("dp", ("tp", "tp2"))),
        check_vma=False,
    )
```

```python
import functools

import jax
import jax.numpy as jnp
from jax import lax
from jax.experimental import pallas as pl
from jax.experimental.pallas import tpu as pltpu
from jax.sharding import PartitionSpec as P

NORM_EPS = 1e-6
ROWS = 128
LANES = 128
MESH = pl.DeviceIdType.MESH


class Sems:
    def __init__(self, ref):
        self.ref, self.used = ref, 0

    def take(self):
        self.used += 1
        return self.ref.at[self.used - 1]


def kernel(
    n2, n1,
    hidden, w_gate, w_up, w_down, gain_in, w_vocab, temp_in, target_in,
    out_row, out_lp,
    hid, wg, wu, wd, wv, acc_g, acc_u, act_t, yp, pair, chip, xr, ys, sq, xs,
    lg, far, mrg, dct, sq_col, sq_all, st_a, st_b, gain, temp, target, row_out, lp_out,
    load_sems, send_sems, recv_sems, cast_sems,
):
    chunks, _, d_model = hid.shape
    ff_own = wg.shape[0]
    d_local = wd.shape[1]
    half = d_local // 2
    v_own = out_lp.shape[0]
    n_x = n1 // 2
    blk = ROWS // n_x
    y = lax.axis_index("tp2")
    tp = lax.axis_index("tp")
    x, core = tp // 2, tp % 2
    loads, sends, recvs = Sems(load_sems), Sems(send_sems), Sems(recv_sems)
    sent = []

    def at_y(j):
        return {"tp2": (y + j) % n2}

    def at_x(j):
        return {"tp": ((x + j) % n_x) * 2 + core}

    partner = {"tp": x * 2 + (1 - core)}

    def remote(src, dst, device):
        return pltpu.make_async_remote_copy(
            src_ref=src, dst_ref=dst, send_sem=sends.take(), recv_sem=recvs.take(),
            device_id=device, device_id_type=MESH,
        )

    def send(copy):
        copy.start()
        sent.append(copy)

    everyone = sorted(
        [(j2, j1) for j2 in range(n2) for j1 in range(n1)][1:],
        key=lambda j: -min(j[0], n2 - j[0]) - min(j[1] // 2, n_x - j[1] // 2),
    )
    casts = []

    def slot_of(y_from, tp_from):
        return ((y + n2 - y_from) % n2) * n1 + (tp + n1 - tp_from) % n1

    def broadcast(buf, index):
        for j2, j1 in everyone:
            pltpu.make_async_remote_copy(
                src_ref=buf.at[0], dst_ref=buf.at[j2 * n1 + j1],
                send_sem=cast_sems.at[index, 0], recv_sem=cast_sems.at[index, 1],
                device_id={"tp2": (y + j2) % n2, "tp": (tp + j1) % n1}, device_id_type=MESH,
            ).start()
        casts.append((buf, index))

    def wait_cast(buf, index, side):
        rest = buf.at[pl.ds(1, n2 * n1 - 1)]
        pltpu.make_async_copy(rest, rest, cast_sems.at[index, side]).wait()

    ff_cut = (ff_own // 2) // 16 * 16
    v_cut = (v_own // 2) // 8 * 8

    def act_rows(i, q, lo, size):
        return act_t.at[i, pl.ds(pl.multiple_of(q * ff_own + lo, 16), size), :]

    def q_of(slot):
        return (y + slot) % n2

    def base_of(slot):
        return pl.multiple_of((v_own * q_of(slot)) // 16 * 16, 16)

    def off_of(slot):
        return pl.multiple_of((v_own * q_of(slot)) % 16, 8)

    def lg_part(i, slot, part):
        lo, size = (0, v_cut) if part == 0 else (v_cut, v_own - v_cut)
        return lg.at[i, slot, pl.ds(pl.multiple_of(off_of(slot) + lo, 8), size), :]

    def part_of(buf, i, part):
        return buf.at[i, part, pl.ds(0, v_cut if part == 0 else v_own - v_cut), :]

    def pieces(i, slot, part, buf):
        lo, size = (0, v_cut) if part == 0 else (v_cut, v_own - v_cut)
        cut = size // 2 // 8 * 8 if i == 0 else size
        for at, n in ((0, cut), (cut, size - cut)):
            if n > 0:
                src = pl.ds(pl.multiple_of(off_of(slot) + lo + at, 8), n)
                yield lg.at[i, slot, src, :], buf.at[i, part, pl.ds(at, n), :]

    x_order = [n_x // 2] + [j for j in range(1, n_x) if j != n_x // 2]

    cps = []
    for i in range(chunks):
        c = {}
        own = act_rows(i, y, 0, ff_own)
        c["own_up"] = remote(own, own, at_y(1))
        c["own_dn"] = remote(own, own, at_y(-1))
        prev, nxt = (y + n2 - 1) % n2, (y + 1) % n2
        lo_half = act_rows(i, prev, 0, ff_cut)
        hi_half = act_rows(i, nxt, ff_cut, ff_own - ff_cut)
        if i == 0:
            lo_half = act_rows(i, y, 0, ff_cut)
            hi_half = act_rows(i, y, ff_cut, ff_own - ff_cut)
            c["fwd_up"] = remote(lo_half, lo_half, at_y(2))
            c["fwd_dn"] = remote(hi_half, hi_half, at_y(-2))
        else:
            c["fwd_up"] = remote(lo_half, lo_half, at_y(1))
            c["fwd_dn"] = remote(hi_half, hi_half, at_y(-1))
        c["pair"] = remote(yp.at[i, 1 - core], pair.at[i], partner)
        c["xrs"] = [
            remote(
                chip.at[i, pl.ds(pl.multiple_of(((x + j) % n_x) * blk, blk), blk), :],
                xr.at[i, j - 1], at_x(j),
            )
            for j in x_order
        ]
        mine = ys.at[i, core, pl.ds(pl.multiple_of(x * blk, blk), blk), :]
        c["xag"] = [remote(mine, mine, at_x(j)) for j in x_order]
        c["swap"] = remote(ys.at[i, core], ys.at[i, core], partner)
        c["ssq"] = [] if i == 0 else [remote(sq.at[i, 0], sq.at[i, j], at_y(j)) for j in range(1, n2)]
        c["far_a"] = remote(lg_part(i, 2, 0), part_of(far, i, 0), at_y(-1))
        c["far_b"] = remote(lg_part(i, 2, 1), part_of(far, i, 1), at_y(1))
        c["dir_a"] = [remote(a, b, at_y(1)) for a, b in pieces(i, 1, 0, dct)]
        c["dir_b"] = [remote(a, b, at_y(-1)) for a, b in pieces(i, 3, 1, dct)]
        c["mrg_a"] = remote(lg_part(i, 3, 0), part_of(mrg, i, 0), at_y(-1))
        c["mrg_b"] = remote(lg_part(i, 1, 1), part_of(mrg, i, 1), at_y(1))
        cps.append(c)

    k_blocks = 5 if d_model % (5 * LANES) == 0 else 4
    kb = d_model // k_blocks

    def load(src, dst):
        return pltpu.make_async_copy(src, dst, loads.take())

    ld_hid = [load(hidden.at[pl.ds(i * ROWS, ROWS), :], hid.at[i]) for i in range(chunks)]
    ld_w = [
        (
            load(w_gate.at[:, pl.ds(k * kb, kb)], wg.at[:, pl.ds(k * kb, kb)]),
            load(w_up.at[:, pl.ds(k * kb, kb)], wu.at[:, pl.ds(k * kb, kb)]),
        )
        for k in range(k_blocks)
    ]
    ld_wd = load(w_down, wd)
    ld_wv = load(w_vocab, wv)
    ld_small = [load(gain_in, gain), load(temp_in, temp), load(target_in, target)]
    peers = [{"tp2": (y + j2) % n2, "tp": (tp + j1) % n1} for j2, j1 in everyone]
    with jax.named_scope("start"):
        ld_hid[0].start()
        for pair_of in ld_w[:1]:
            for cp in pair_of:
                cp.start()
        for cp in ld_hid[1:2]:
            cp.start()
        for pair_of in ld_w[1:]:
            for cp in pair_of:
                cp.start()
        for cp in ld_small:
            cp.start()
        barrier = pltpu.get_barrier_semaphore()
        for device in peers:
            pl.semaphore_signal(barrier, inc=1, device_id=device, device_id_type=MESH)

    NT = (((1,), (1,)), ((), ()))

    def gate_up(first, count):
        for i in range(first, first + count):
            ld_hid[i].wait()
        for k in range(k_blocks):
            cols = pl.ds(k * kb, kb)
            if first == 0 and k == k_blocks - 1:
                for cp in ld_hid[2:]:
                    cp.start()
            if first == 0:
                for cp in ld_w[k]:
                    cp.wait()
            h = hid[first:first + count, :, cols].reshape(count * ROWS, kb)
            g = lax.dot_general(wg[:, cols], h, NT, preferred_element_type=jnp.float32)
            u = lax.dot_general(wu[:, cols], h, NT, preferred_element_type=jnp.float32)
            if k == 0:
                acc_g[...] = g
                acc_u[...] = u
            else:
                acc_g[...] += g
                acc_u[...] += u
        act = (jax.nn.silu(acc_g[...]) * acc_u[...]).astype(jnp.bfloat16)
        for i in range(count):
            act_t[first + i, pl.ds(pl.multiple_of(y * ff_own, 16), ff_own), :] = (
                act[:, i * ROWS:(i + 1) * ROWS]
            )

    def send_own(i):
        send(cps[i]["own_up"])
        send(cps[i]["own_dn"])
        if i == 0:
            send(cps[i]["fwd_up"])
            send(cps[i]["fwd_dn"])

    def forward(i):
        cps[i]["own_up"].wait_recv()
        send(cps[i]["fwd_up"])
        cps[i]["own_dn"].wait_recv()
        send(cps[i]["fwd_dn"])

    def down(i):
        if i == 0:
            cps[i]["own_up"].wait_recv()
            cps[i]["own_dn"].wait_recv()
        cps[i]["fwd_up"].wait_recv()
        cps[i]["fwd_dn"].wait_recv()
        if i == 0:
            ld_wd.wait()
        for s in range(2):
            yp[i, s] = lax.dot_general(
                act_t[i], wd[:, s * half:(s + 1) * half],
                (((0,), (0,)), ((), ())), preferred_element_type=jnp.float32,
            ).astype(jnp.bfloat16)
        send(cps[i]["pair"])

    def chip_sum(i):
        cps[i]["pair"].wait_recv()
        chip[i] = (
            yp[i, core].astype(jnp.float32) + pair[i].astype(jnp.float32)
        ).astype(jnp.bfloat16)
        for cp in cps[i]["xrs"]:
            send(cp)

    def row_sum(i):
        at = pl.ds(pl.multiple_of(x * blk, blk), blk)
        total = chip[i, at, :].astype(jnp.float32)
        for j, cp in zip(x_order, cps[i]["xrs"]):
            cp.wait_recv()
            total += xr[i, j - 1].astype(jnp.float32)
        total = total.astype(jnp.bfloat16)
        ys[i, core, at, :] = total
        for cp in cps[i]["xag"]:
            send(cp)
        if i == 0:
            cols = pl.ds(pl.multiple_of(y * d_local + core * half, LANES), half)
            r = hid[i, at, cols].astype(jnp.float32) + total.astype(jnp.float32)
            part = jnp.sum(r * r, axis=1, keepdims=True)
            sq_col[...] = jnp.zeros_like(sq_col)
            sq_col[at, :] = jnp.broadcast_to(part, (blk, LANES))
            sq_all[0] = sq_col[...].T[:8, :]
            broadcast(sq_all, 0)

    def swap(i):
        for cp in cps[i]["xag"]:
            cp.wait_recv()
        send(cps[i]["swap"])

    def residual(i, s):
        cols = pl.ds(pl.multiple_of(y * d_local + s * half, LANES), half)
        return hid[i, :, cols].astype(jnp.float32) + ys[i, s].astype(jnp.float32)

    def square(i):
        cps[i]["swap"].wait_recv()
        part = 0.0
        for s in range(2):
            r = residual(i, s)
            part = part + jnp.sum(r * r, axis=1, keepdims=True)
        sq[i, 0] = jnp.broadcast_to(part, (ROWS, LANES)).T[:8, :]
        for cp in cps[i]["ssq"]:
            send(cp)

    def norm(i):
        if i == 0:
            cps[i]["swap"].wait_recv()
            wait_cast(sq_all, 0, 1)
            total = jnp.sum(sq_all[...], axis=0)
        else:
            total = sq[i, 0]
            for j, cp in enumerate(cps[i]["ssq"]):
                cp.wait_recv()
                total = total + sq[i, j + 1]
        inv = lax.rsqrt(total / d_model + NORM_EPS)
        inv = jnp.broadcast_to(inv[:1, :], (LANES, ROWS)).T[:, :1]
        for s in range(2):
            g = gain[:, pl.ds(pl.multiple_of(y * d_local + s * half, LANES), half)]
            xs[i, :, s * half:(s + 1) * half] = (g * residual(i, s) * inv).astype(jnp.bfloat16)

    window = lg.shape[2]
    step = window // 3 if window % 48 == 0 else window

    def logits(i, slot):
        base = base_of(slot)

        @pl.loop(0, window // step)
        def _(j):
            at = pl.multiple_of(j * step, 16)
            lg[i, slot, pl.ds(at, step), :] = lax.dot_general(
                wv[pl.ds(pl.multiple_of(base + at, 16), step), :], xs[i], NT,
                preferred_element_type=jnp.float32,
            )

    def logits_far(i):
        logits(i, 2)
        send(cps[i]["far_a"])
        send(cps[i]["far_b"])

    def logits_near(i):
        logits(i, 1)
        send(cps[i]["dir_a"][0])
        logits(i, 3)
        send(cps[i]["dir_b"][0])

    def near_send(i):
        send(cps[i]["dir_a"][1])
        send(cps[i]["dir_b"][1])

    def merge(i):
        for name, slot, part in (("a", 3, 0), ("b", 1, 1)):
            cps[i]["far_" + name].wait_recv()
            lg_part(i, slot, part)[...] += part_of(far, i, part)[...]
            send(cps[i]["mrg_" + name])

    def own(i):
        logits(i, 0)

    def near_sum(i):
        for part in range(2):
            for cp in cps[i]["dir_" + "ab"[part]]:
                cp.wait_recv()
            lg_part(i, 0, part)[...] += part_of(dct, i, part)[...]

    def finish(i):
        lanes = pl.ds(i * ROWS, ROWS)
        t = temp[:, lanes]
        tgt = target[:, lanes]
        col0 = (tp * n2 + y) * v_own
        peak = None
        for part in range(2):
            cps[i]["mrg_" + "ab"[part]].wait_recv()
            ref = lg_part(i, 0, part)
            val = (ref[...] + part_of(mrg, i, part)[...]) / t
            ref[...] = val
            top = jnp.max(val, axis=0, keepdims=True)
            peak = top if peak is None else jnp.maximum(peak, top)
        total = dot = hit = 0.0
        for part in range(2):
            val = lg_part(i, 0, part)[...]
            e = jnp.exp(val - peak)
            total = total + jnp.sum(e, axis=0, keepdims=True)
            dot = dot + jnp.sum(e * val, axis=0, keepdims=True)
            ids = col0 + part * v_cut + lax.broadcasted_iota(jnp.int32, val.shape, 0)
            hit = hit + jnp.sum(jnp.where(ids == tgt, val, 0.0), axis=0, keepdims=True)
        buf, at = (st_b, slice(0, ROWS)) if i == chunks - 1 else (st_a, lanes)
        for row, v in enumerate((peak, total, dot, hit)):
            buf[0, row, :, at] = v

    def combine(buf, lanes):
        peak = jnp.max(buf[:, 0], axis=0)
        total = dot = hit = 0.0
        for j2 in range(n2):
            for j1 in range(n1):
                v = buf[slot_of(j2, j1)]
                scale = jnp.exp(v[0] - peak)
                total = total + v[1] * scale
                dot = dot + v[2] * scale
                hit = hit + v[3]
        log_norm = peak + jnp.log(total)
        row_out[0:1, lanes] = log_norm
        row_out[1:2, lanes] = log_norm - dot / total
        row_out[2:3, lanes] = hit - log_norm

    def output(first, count):
        for i in range(first, first + count):
            lanes = slice(i * ROWS, (i + 1) * ROWS)
            val = lg[i, 0, pl.ds(off_of(0), v_own), :]
            lp_out[:, lanes] = (val - row_out[0:1, lanes]).astype(jnp.bfloat16)

    last = chunks - 1

    def run(*items):
        for fn, i in items:
            if 0 <= i <= last:
                with jax.named_scope(f"{fn.__name__}#c={i}"):
                    fn(i)

    def produce(i):
        gate_up(i, pack)

    pack = acc_g.shape[1] // ROWS
    run((produce, 0))
    with jax.named_scope("barrier"):
        pl.semaphore_wait(barrier, len(peers))
    run((send_own, 0))
    ld_wd.start()
    run((send_own, 1))
    ld_wv.start()
    for i in range(pack, chunks, pack):
        run((produce, i))
    for cp in ld_small:
        cp.wait()
    run((send_own, 2), (down, 0), (chip_sum, 0), (forward, 1), (row_sum, 0), (send_own, 3))
    run((forward, 2), (down, 1), (swap, 0), (chip_sum, 1), (norm, 0), (forward, 3))
    ld_wv.wait()
    run((logits_far, 0), (logits_near, 0), (row_sum, 1), (down, 2), (down, 3), (chip_sum, 2))
    run((chip_sum, 3), (swap, 1), (square, 1), (near_send, 0), (row_sum, 2), (norm, 1))
    run((logits_far, 1), (row_sum, 3), (swap, 2), (square, 2), (merge, 0), (logits_near, 1))
    run((swap, 3), (square, 3), (norm, 2))
    for i in range(1, chunks - 1):
        run((logits_far, i + 1), (merge, i), (logits_near, i + 1), (norm, i + 2))
        run((own, i - 1), (near_sum, i - 1))
    run((finish, last - 3), (own, last - 1), (own, last), (near_sum, last - 1), (finish, last - 2))
    run((merge, last), (finish, last - 1))
    with jax.named_scope("cast_a"):
        broadcast(st_a, 1)
    run((near_sum, last), (finish, last))
    with jax.named_scope("cast_b"):
        broadcast(st_b, 2)
    with jax.named_scope("output_a"):
        wait_cast(st_a, 1, 1)
        combine(st_a, slice(0, last * ROWS))
        output(0, last)
        first_store = load(lp_out.at[:, :last * ROWS], out_lp.at[:, :last * ROWS])
        first_store.start()
    with jax.named_scope("sent"):
        for cp in sent:
            cp.wait_send()
    with jax.named_scope("wait_b"):
        wait_cast(st_b, 2, 1)
    with jax.named_scope("output_b"):
        combine(st_b, slice(last * ROWS, chunks * ROWS))
        output(last, 1)
    with jax.named_scope("drain"):
        stores = [load(row_out, out_row), load(lp_out.at[:, last * ROWS:], out_lp.at[:, last * ROWS:])]
        for cp in stores:
            cp.start()
        for buf, index in casts:
            wait_cast(buf, index, 0)
        for cp in [first_store] + stores:
            cp.wait()


def emit(rows_in, lp_in, ln, ent, tgt, lp):
    ln[...] = rows_in[0:1, :]
    ent[...] = rows_in[1:2, :]
    tgt[...] = rows_in[2:3, :]
    lp[...] = lp_in[...]


def solution(mesh):
    n2, n1 = mesh.shape["tp2"], mesh.shape["tp"]

    def device_step(hidden, w_gate, w_up, w_down, norm_gain, w_vocab, temperature, target):
        rows, d_model = hidden.shape
        ff_own = w_gate.shape[1]
        ff_tp, d_local = w_down.shape
        v_tp = w_vocab.shape[1]
        v_own = v_tp // n2
        chunks = rows // ROWS
        half = d_local // 2
        n_x = n1 // 2
        blk = ROWS // n_x
        pack = min(2, chunks)
        window = -(-v_own // 16) * 16
        part = v_own - (v_own // 2) // 8 * 8
        bf, f32 = jnp.bfloat16, jnp.float32
        n_loads = chunks + 10 + 2 + 3 + 3
        n_copies = 2 + chunks * (4 + 1 + (n_x - 1) * 2 + 1 + 6) + (chunks - 1) * (n2 - 1)
        row = lambda a: a.reshape(1, -1)
        vmem = pl.BlockSpec(memory_space=pltpu.VMEM)
        hbm = pl.BlockSpec(memory_space=pl.ANY)
        results = [
            jax.ShapeDtypeStruct((1, rows), f32),
            jax.ShapeDtypeStruct((1, rows), f32),
            jax.ShapeDtypeStruct((1, rows), f32),
            jax.ShapeDtypeStruct((v_own, rows), bf),
        ]
        parts = pl.pallas_call(
            functools.partial(kernel, n2, n1),
            out_shape=[jax.ShapeDtypeStruct((8, rows), f32), results[3]],
            in_specs=[hbm] * 8,
            out_specs=[hbm, hbm],
            scratch_shapes=[
                pltpu.VMEM((chunks, ROWS, d_model), bf),
                pltpu.VMEM((ff_own, d_model), bf),
                pltpu.VMEM((ff_own, d_model), bf),
                pltpu.VMEM((ff_tp, d_local), bf),
                pltpu.VMEM((v_tp, d_local), bf),
                pltpu.VMEM((ff_own, pack * ROWS), f32),
                pltpu.VMEM((ff_own, pack * ROWS), f32),
                pltpu.VMEM((chunks, ff_tp, ROWS), bf),
                pltpu.VMEM((chunks, 2, ROWS, half), bf),
                pltpu.VMEM((chunks, ROWS, half), bf),
                pltpu.VMEM((chunks, ROWS, half), bf),
                pltpu.VMEM((chunks, n_x - 1, blk, half), bf),
                pltpu.VMEM((chunks, 2, ROWS, half), bf),
                pltpu.VMEM((chunks, n2, 8, ROWS), f32),
                pltpu.VMEM((chunks, ROWS, d_local), bf),
                pltpu.VMEM((chunks, n2, window, ROWS), f32),
                pltpu.VMEM((chunks, 2, part, ROWS), f32),
                pltpu.VMEM((chunks, 2, part, ROWS), f32),
                pltpu.VMEM((chunks, 2, part, ROWS), f32),
                pltpu.VMEM((ROWS, LANES), f32),
                pltpu.VMEM((n2 * n1, 8, ROWS), f32),
                pltpu.VMEM((n2 * n1, 4, 1, rows - ROWS), f32),
                pltpu.VMEM((n2 * n1, 4, 1, ROWS), f32),
                pltpu.VMEM((1, d_model), f32),
                pltpu.VMEM((1, rows), f32),
                pltpu.VMEM((1, rows), jnp.int32),
                pltpu.VMEM((8, rows), f32),
                pltpu.VMEM((v_own, rows), bf),
                pltpu.SemaphoreType.DMA((n_loads,)),
                pltpu.SemaphoreType.DMA((n_copies,)),
                pltpu.SemaphoreType.DMA((n_copies,)),
                pltpu.SemaphoreType.DMA((3, 2)),
            ],
            compiler_params=pltpu.CompilerParams(
                collective_id=0, has_side_effects=True, vmem_limit_bytes=66_000_000,
            ),
            name="decode_tail",
        )(
            hidden, w_gate.T, w_up.T, w_down, row(norm_gain), w_vocab.T,
            row(temperature), row(target),
        )
        ln, ent, tgt, lp = pl.pallas_call(
            emit, out_shape=results, in_specs=[vmem] * 2, out_specs=[vmem] * 4, name="emit",
        )(*parts)
        return ln.reshape(rows), ent.reshape(rows), tgt.reshape(rows), lp.T

    return jax.shard_map(
        device_step, mesh=mesh,
        in_specs=(
            P("dp", None), P(None, ("tp", "tp2")), P(None, ("tp", "tp2")), P("tp", "tp2"),
            P(None), P("tp2", "tp"), P("dp"), P("dp"),
        ),
        out_specs=(P("dp"), P("dp"), P("dp"), P("dp", ("tp", "tp2"))),
        check_vma=False,
    )
```

```python
import functools

import jax
import jax.numpy as jnp
from jax import lax
from jax.experimental import pallas as pl
from jax.experimental.pallas import tpu as pltpu
from jax.sharding import PartitionSpec as P

NORM_EPS = 1e-6
ROWS = 128
LANES = 128
MESH = pl.DeviceIdType.MESH


class Sems:
    def __init__(self, ref):
        self.ref, self.used = ref, 0

    def take(self):
        self.used += 1
        return self.ref.at[self.used - 1]


def kernel(
    n2, n1, pack,
    hidden, w_gate, w_up, w_down, gain_in, w_vocab, temp_in, target_in,
    out_ln, out_ent, out_tgt, out_lp,
    hid, wgu, wd, wv, act_t, yp, pair, chip, xr, ys, sq, xs,
    lg, far, mrg, dct, sq_col, sq_all, st_a, st_y, st_b, gain, temp, target, ln, ent, tgt_lp, lp_out,
    load_sems, send_sems, recv_sems, cast_sems,
):
    chunks, _, d_model = hid.shape
    thirds, ff_part = wgu.shape[0], wgu.shape[1] // 2
    ff_own = thirds * ff_part
    d_local = wd.shape[1]
    half = d_local // 2
    v_own = out_lp.shape[0]
    n_x = n1 // 2
    blk = ROWS // n_x
    y = lax.axis_index("tp2")
    tp = lax.axis_index("tp")
    x, core = tp // 2, tp % 2
    loads, sends, recvs = Sems(load_sems), Sems(send_sems), Sems(recv_sems)
    sent = []

    def at_y(j):
        return {"tp2": (y + j) % n2}

    def at_x(j):
        return {"tp": ((x + j) % n_x) * 2 + core}

    partner = {"tp": x * 2 + (1 - core)}

    def remote(src, dst, device):
        return pltpu.make_async_remote_copy(
            src_ref=src, dst_ref=dst, send_sem=sends.take(), recv_sem=recvs.take(),
            device_id=device, device_id_type=MESH,
        )

    def send(copy):
        copy.start()
        sent.append(copy)

    everyone = sorted(
        [(j2, j1) for j2 in range(n2) for j1 in range(n1)][1:],
        key=lambda j: -min(j[0], n2 - j[0]) - min(j[1] // 2, n_x - j[1] // 2),
    )

    def slot_of(y_from, tp_from):
        return ((y + n2 - y_from) % n2) * n1 + (tp + n1 - tp_from) % n1

    def broadcast(buf, index):
        for j2, j1 in everyone:
            pltpu.make_async_remote_copy(
                src_ref=buf.at[0], dst_ref=buf.at[j2 * n1 + j1],
                send_sem=cast_sems.at[index, 0], recv_sem=cast_sems.at[index, 1],
                device_id={"tp2": (y + j2) % n2, "tp": (tp + j1) % n1}, device_id_type=MESH,
            ).start()

    def wait_cast(buf, index, side):
        rest = buf.at[pl.ds(1, n2 * n1 - 1)]
        pltpu.make_async_copy(rest, rest, cast_sems.at[index, side]).wait()

    ff_cut = (ff_own // 2) // 16 * 16
    v_cut = (v_own // 2) // 8 * 8

    def act_rows(i, q, lo, size):
        return act_t.at[i, pl.ds(pl.multiple_of(q * ff_own + lo, 16), size), :]

    def q_of(slot):
        return (y + slot) % n2

    def base_of(slot):
        return pl.multiple_of((v_own * q_of(slot)) // 16 * 16, 16)

    def off_of(slot):
        return pl.multiple_of((v_own * q_of(slot)) % 16, 8)

    def lg_part(i, slot, part):
        lo, size = (0, v_cut) if part == 0 else (v_cut, v_own - v_cut)
        return lg.at[i, slot, pl.ds(pl.multiple_of(off_of(slot) + lo, 8), size), :]

    def part_of(buf, i, part):
        return buf.at[i, part, pl.ds(0, v_cut if part == 0 else v_own - v_cut), :]

    def pieces(i, slot, part, buf):
        lo, size = (0, v_cut) if part == 0 else (v_cut, v_own - v_cut)
        cut = size // 2 // 8 * 8 if i == 0 else size
        for at, n in ((0, cut), (cut, size - cut)):
            if n > 0:
                src = pl.ds(pl.multiple_of(off_of(slot) + lo + at, 8), n)
                yield lg.at[i, slot, src, :], buf.at[i, part, pl.ds(at, n), :]

    x_order = [n_x // 2] + [j for j in range(1, n_x) if j != n_x // 2]

    cps = []
    for i in range(chunks):
        c = {}
        parts = thirds if i == 0 else 1
        own = [act_rows(i, y, t * (ff_own // parts), ff_own // parts) for t in range(parts)]
        c["own_up"] = [remote(a, a, at_y(1)) for a in own]
        c["own_dn"] = [remote(a, a, at_y(-1)) for a in own]
        prev, nxt = (y + n2 - 1) % n2, (y + 1) % n2
        lo_half = act_rows(i, prev, 0, ff_cut)
        hi_half = act_rows(i, nxt, ff_cut, ff_own - ff_cut)
        if i == 0:
            c["own_far"] = [remote(a, a, at_y(2)) for a in own]
        else:
            c["fwd_up"] = remote(lo_half, lo_half, at_y(1))
            c["fwd_dn"] = remote(hi_half, hi_half, at_y(-1))
        c["pair"] = remote(yp.at[i, 1 - core], pair.at[i], partner)
        c["xrs"] = [
            remote(
                chip.at[i, pl.ds(pl.multiple_of(((x + j) % n_x) * blk, blk), blk), :],
                xr.at[i, j - 1], at_x(j),
            )
            for j in x_order
        ]
        mine = ys.at[i, core, pl.ds(pl.multiple_of(x * blk, blk), blk), :]
        c["xag"] = [remote(mine, mine, at_x(j)) for j in x_order]
        c["swap"] = remote(ys.at[i, core], ys.at[i, core], partner)
        c["ssq"] = [] if i == 0 else [remote(sq.at[i, 0], sq.at[i, j], at_y(j)) for j in range(1, n2)]
        c["far_a"] = remote(lg_part(i, 2, 0), part_of(far, i, 0), at_y(-1))
        c["far_b"] = remote(lg_part(i, 2, 1), part_of(far, i, 1), at_y(1))
        c["dir_a"] = [remote(a, b, at_y(1)) for a, b in pieces(i, 1, 0, dct)]
        c["dir_b"] = [remote(a, b, at_y(-1)) for a, b in pieces(i, 3, 1, dct)]
        c["mrg_a"] = remote(lg_part(i, 3, 0), part_of(mrg, i, 0), at_y(-1))
        c["mrg_b"] = remote(lg_part(i, 1, 1), part_of(mrg, i, 1), at_y(1))
        cps.append(c)

    cp_tp = [remote(st_a.at[0], st_a.at[j], {"tp": (tp + j) % n1}) for j in range(n1 - 1, 0, -1)]
    cp_y = [remote(st_y.at[0], st_y.at[j], at_y(j)) for j in range(1, n2)]

    def load(src, dst):
        return pltpu.make_async_copy(src, dst, loads.take())

    ld_hid = [load(hidden.at[pl.ds(i * ROWS, ROWS), :], hid.at[i]) for i in range(chunks)]
    ld_w = [
        [
            load(w.at[pl.ds(t * ff_part, ff_part), :], wgu.at[t, pl.ds(side * ff_part, ff_part), :])
            for side, w in enumerate((w_gate, w_up))
        ]
        for t in range(thirds)
    ]
    ld_wd = load(w_down, wd)
    ld_wv = load(w_vocab, wv)
    ld_small = [load(gain_in, gain), load(temp_in, temp), load(target_in, target)]
    peers = [{"tp2": (y + j2) % n2, "tp": (tp + j1) % n1} for j2, j1 in everyone]
    with jax.named_scope("start"):
        for cp in ld_hid[:pack] + [cp for both in ld_w for cp in both]:
            cp.start()
        for cp in ld_small:
            cp.start()
        barrier = pltpu.get_barrier_semaphore()
        for device in peers:
            pl.semaphore_signal(barrier, inc=1, device_id=device, device_id_type=MESH)

    NT = (((1,), (1,)), ((), ()))

    def gate_up(first, t):
        r = lax.dot_general(
            wgu[t], hid[first:first + pack].reshape(pack * ROWS, d_model), NT,
            preferred_element_type=jnp.float32,
        )
        act = (jax.nn.silu(r[:ff_part]) * r[ff_part:]).astype(jnp.bfloat16)
        for i in range(pack):
            at = pl.ds(pl.multiple_of(y * ff_own + t * ff_part, 16), ff_part)
            act_t[first + i, at, :] = act[:, i * ROWS:(i + 1) * ROWS]

    def send_own(i, t=0):
        send(cps[i]["own_up"][t])
        if i == 0:
            send(cps[i]["own_far"][t])
        send(cps[i]["own_dn"][t])

    def forward(i):
        cps[i]["own_up"][0].wait_recv()
        send(cps[i]["fwd_up"])
        cps[i]["own_dn"][0].wait_recv()
        send(cps[i]["fwd_dn"])

    def down(i):
        names = ("own_up", "own_dn", "own_far") if i == 0 else ()
        for cp in [cp for name in names for cp in cps[i][name]]:
            cp.wait_recv()
        if i > 0:
            cps[i]["fwd_up"].wait_recv()
            cps[i]["fwd_dn"].wait_recv()
        if i == 0:
            ld_wd.wait()
        for s in range(2):
            yp[i, s] = lax.dot_general(
                act_t[i], wd[:, s * half:(s + 1) * half],
                (((0,), (0,)), ((), ())), preferred_element_type=jnp.float32,
            ).astype(jnp.bfloat16)
        send(cps[i]["pair"])

    def chip_sum(i):
        cps[i]["pair"].wait_recv()
        chip[i] = (
            yp[i, core].astype(jnp.float32) + pair[i].astype(jnp.float32)
        ).astype(jnp.bfloat16)
        for cp in cps[i]["xrs"]:
            send(cp)

    def row_sum(i):
        at = pl.ds(pl.multiple_of(x * blk, blk), blk)
        total = chip[i, at, :].astype(jnp.float32)
        for j, cp in zip(x_order, cps[i]["xrs"]):
            cp.wait_recv()
            total += xr[i, j - 1].astype(jnp.float32)
        total = total.astype(jnp.bfloat16)
        ys[i, core, at, :] = total
        for cp in cps[i]["xag"]:
            send(cp)
        if i == 0:
            cols = pl.ds(pl.multiple_of(y * d_local + core * half, LANES), half)
            r = hid[i, at, cols].astype(jnp.float32) + total.astype(jnp.float32)
            part = jnp.sum(r * r, axis=1, keepdims=True)
            sq_col[...] = jnp.zeros_like(sq_col)
            sq_col[at, :] = jnp.broadcast_to(part, (blk, LANES))
            sq_all[0] = sq_col[...].T[:8, :]
            broadcast(sq_all, 0)

    def swap(i):
        for cp in cps[i]["xag"]:
            cp.wait_recv()
        send(cps[i]["swap"])

    def residual(i, s):
        cols = pl.ds(pl.multiple_of(y * d_local + s * half, LANES), half)
        return hid[i, :, cols].astype(jnp.float32) + ys[i, s].astype(jnp.float32)

    def square(i):
        cps[i]["swap"].wait_recv()
        part = 0.0
        for s in range(2):
            r = residual(i, s)
            part = part + jnp.sum(r * r, axis=1, keepdims=True)
        sq[i, 0] = jnp.broadcast_to(part, (ROWS, LANES)).T[:8, :]
        for cp in cps[i]["ssq"]:
            send(cp)

    def norm(i):
        if i == 0:
            cps[i]["swap"].wait_recv()
            wait_cast(sq_all, 0, 1)
            total = jnp.sum(sq_all[...], axis=0)
        else:
            total = sq[i, 0]
            for j, cp in enumerate(cps[i]["ssq"]):
                cp.wait_recv()
                total = total + sq[i, j + 1]
        inv = lax.rsqrt(total / d_model + NORM_EPS)
        inv = jnp.broadcast_to(inv[:1, :], (LANES, ROWS)).T[:, :1]
        for s in range(2):
            g = gain[:, pl.ds(pl.multiple_of(y * d_local + s * half, LANES), half)]
            xs[i, :, s * half:(s + 1) * half] = (g * residual(i, s) * inv).astype(jnp.bfloat16)

    window = lg.shape[2]
    step = window // 3 if window % 48 == 0 else window

    def piece(i, slot, at, size):
        lg[i, slot, pl.ds(at, size), :] = lax.dot_general(
            wv[pl.ds(pl.multiple_of(base_of(slot) + at, 16), size), :], xs[i], NT,
            preferred_element_type=jnp.float32,
        )

    def logits(i, slot):
        @pl.loop(0, window // step)
        def _(j):
            piece(i, slot, pl.multiple_of(j * step, 16), step)

    def logits_far(i):
        if i == 0:
            cut = -(-(v_cut + 8) // 16) * 16
            piece(i, 2, 0, cut)
            send(cps[i]["far_a"])
            piece(i, 2, cut, window - cut)
        else:
            logits(i, 2)
            send(cps[i]["far_a"])
        send(cps[i]["far_b"])

    def logits_near(i):
        logits(i, 1)
        send(cps[i]["dir_a"][0])
        logits(i, 3)
        send(cps[i]["dir_b"][0])

    def near_send(i):
        send(cps[i]["dir_a"][1])
        send(cps[i]["dir_b"][1])

    def merge(i):
        for name, slot, part in (("a", 3, 0), ("b", 1, 1)):
            cps[i]["far_" + name].wait_recv()
            lg_part(i, slot, part)[...] += part_of(far, i, part)[...]
            send(cps[i]["mrg_" + name])

    def own(i):
        logits(i, 0)

    def near_sum(i):
        for part in range(2):
            for cp in cps[i]["dir_" + "ab"[part]]:
                cp.wait_recv()
            lg_part(i, 0, part)[...] += part_of(dct, i, part)[...]

    def finish(i):
        lanes = pl.ds(i * ROWS, ROWS)
        t = temp[:, lanes]
        tgt = target[:, lanes]
        col0 = (tp * n2 + y) * v_own
        peak = None
        for part in range(2):
            cps[i]["mrg_" + "ab"[part]].wait_recv()
            ref = lg_part(i, 0, part)
            val = (ref[...] + part_of(mrg, i, part)[...]) / t
            ref[...] = val
            top = jnp.max(val, axis=0, keepdims=True)
            peak = top if peak is None else jnp.maximum(peak, top)
        total = dot = hit = 0.0
        for part in range(2):
            val = lg_part(i, 0, part)[...]
            e = jnp.exp(val - peak)
            total = total + jnp.sum(e, axis=0, keepdims=True)
            dot = dot + jnp.sum(e * val, axis=0, keepdims=True)
            ids = col0 + part * v_cut + lax.broadcasted_iota(jnp.int32, val.shape, 0)
            hit = hit + jnp.sum(jnp.where(ids == tgt, val, 0.0), axis=0, keepdims=True)
        buf, at = (st_b, slice(0, ROWS)) if i == chunks - 1 else (st_a, lanes)
        for row, v in enumerate((peak, total, dot, hit)):
            buf[0, row, :, at] = v

    def combine(buf, slots):
        peak = jnp.max(buf[:, 0], axis=0)
        total = dot = hit = 0.0
        for slot in slots:
            v = buf[slot]
            scale = jnp.exp(v[0] - peak)
            total = total + v[1] * scale
            dot = dot + v[2] * scale
            hit = hit + v[3]
        return peak, total, dot, hit

    def row_results(stats, lanes):
        peak, total, dot, hit = stats
        log_norm = peak + jnp.log(total)
        ln[:, lanes] = log_norm
        ent[:, lanes] = log_norm - dot / total
        tgt_lp[:, lanes] = hit - log_norm

    def output(first, count):
        for i in range(first, first + count):
            lanes = slice(i * ROWS, (i + 1) * ROWS)
            val = lg[i, 0, pl.ds(off_of(0), v_own), :]
            lp_out[:, lanes] = (val - ln[:, lanes]).astype(jnp.bfloat16)

    last = chunks - 1

    def run(*items):
        for fn, i in items:
            if 0 <= i <= last:
                with jax.named_scope(f"{fn.__name__}#c={i}"):
                    fn(i)

    for cp in ld_hid[:pack]:
        cp.wait()
    for t in range(thirds):
        with jax.named_scope(f"gate_up#c=0#t={t}"):
            for cp in ld_w[t]:
                cp.wait()
            if t == thirds - 1:
                for cp in ld_hid[pack:]:
                    cp.start()
            gate_up(0, t)
        if t == 0:
            with jax.named_scope("barrier"):
                pl.semaphore_wait(barrier, len(peers))
        send_own(0, t)
    ld_wd.start()
    for i in range(1, pack):
        send_own(i)
    ld_wv.start()
    for i in range(pack, chunks, pack):
        for cp in ld_hid[i:i + pack]:
            cp.wait()
        with jax.named_scope(f"gate_up#c={i}"):
            for t in range(thirds):
                gate_up(i, t)
    for cp in ld_small:
        cp.wait()
    run((send_own, 2), (down, 0), (chip_sum, 0), (forward, 1), (row_sum, 0), (send_own, 3))
    run((forward, 2), (down, 1), (swap, 0), (chip_sum, 1), (norm, 0), (forward, 3))
    ld_wv.wait()
    run((logits_far, 0), (logits_near, 0), (row_sum, 1), (down, 2), (down, 3), (chip_sum, 2))
    run((chip_sum, 3), (swap, 1), (square, 1), (near_send, 0), (row_sum, 2), (norm, 1))
    run((logits_far, 1), (row_sum, 3), (swap, 2), (square, 2), (merge, 0), (logits_near, 1))
    run((swap, 3), (square, 3), (norm, 2))
    for i in range(1, chunks - 1):
        run((logits_far, i + 1), (merge, i), (logits_near, i + 1), (norm, i + 2))
        run((own, i - 1), (near_sum, i - 1))
    run((finish, last - 3), (own, last - 1), (own, last), (near_sum, last - 1), (finish, last - 2))
    run((merge, last), (finish, last - 1))
    for cp in cp_tp:
        send(cp)
    run((near_sum, last),)
    with jax.named_scope("stats_tp"):
        for cp in cp_tp:
            cp.wait_recv()
        for row, v in enumerate(combine(st_a, [(tp + n1 - j) % n1 for j in range(n1)])):
            st_y[0, row] = v
        for cp in cp_y:
            send(cp)
    run((finish, last),)
    with jax.named_scope("cast_b"):
        broadcast(st_b, 1)
    with jax.named_scope("output_a"):
        for cp in cp_y:
            cp.wait_recv()
        row_results(combine(st_y, [(y + n2 - j) % n2 for j in range(n2)]), slice(0, last * ROWS))
        output(0, last)
        first_store = load(lp_out.at[:, :last * ROWS], out_lp.at[:, :last * ROWS])
        first_store.start()
    with jax.named_scope("sent"):
        for cp in sent:
            cp.wait_send()
        wait_cast(sq_all, 0, 0)
    with jax.named_scope("wait_b"):
        wait_cast(st_b, 1, 1)
    with jax.named_scope("output_b"):
        order = [slot_of(j2, j1) for j2 in range(n2) for j1 in range(n1)]
        row_results(combine(st_b, order), slice(last * ROWS, chunks * ROWS))
        output(last, 1)
    with jax.named_scope("drain"):
        stores = [load(lp_out.at[:, last * ROWS:], out_lp.at[:, last * ROWS:])]
        stores += [load(a, b) for a, b in ((ln, out_ln), (ent, out_ent), (tgt_lp, out_tgt))]
        for cp in stores:
            cp.start()
        wait_cast(st_b, 1, 0)
        for cp in [first_store] + stores:
            cp.wait()


def emit(*refs):
    ins, outs, bufs, sems = refs[:4], refs[4:8], refs[8:12], refs[12]
    rows = ins[3].shape[0]
    cut = -(-rows // 64) * 16
    pieces = [(3, pl.ds(lo, min(cut, rows - lo))) for lo in range(0, rows, cut)]
    pieces += [(n, pl.ds(0, 1)) for n in range(3)]
    taken = [
        pltpu.make_async_copy(ins[n].at[at, :], bufs[n].at[at, :], sems.at[0, k])
        for k, (n, at) in enumerate(pieces)
    ]
    given = [
        pltpu.make_async_copy(bufs[n].at[at, :], outs[n].at[at, :], sems.at[1, k])
        for k, (n, at) in enumerate(pieces)
    ]
    for cp in taken:
        cp.start()
    for a, b in zip(taken, given):
        a.wait()
        b.start()
    for cp in given:
        cp.wait()


def solution(mesh):
    n2, n1 = mesh.shape["tp2"], mesh.shape["tp"]

    def device_step(hidden, w_gate, w_up, w_down, norm_gain, w_vocab, temperature, target):
        rows, d_model = hidden.shape
        ff_own = w_gate.shape[1]
        ff_tp, d_local = w_down.shape
        v_tp = w_vocab.shape[1]
        v_own = v_tp // n2
        chunks = rows // ROWS
        half = d_local // 2
        n_x = n1 // 2
        blk = ROWS // n_x
        pack = min(2, chunks)
        thirds = 3 if ff_own % 48 == 0 else 1
        window = -(-v_own // 16) * 16
        part = v_own - (v_own // 2) // 8 * 8
        bf, f32 = jnp.bfloat16, jnp.float32
        n_loads = chunks + 6 + 2 + 3 + 5
        n_copies = 2 + 3 * 3 + n1 + n2 + chunks * (4 + 1 + (n_x - 1) * 2 + 1 + 6) + (chunks - 1) * (n2 - 1)
        row = lambda a: a.reshape(1, -1)
        vmem = pl.BlockSpec(memory_space=pltpu.VMEM)
        hbm = pl.BlockSpec(memory_space=pl.ANY)
        results = [
            jax.ShapeDtypeStruct((1, rows), f32),
            jax.ShapeDtypeStruct((1, rows), f32),
            jax.ShapeDtypeStruct((1, rows), f32),
            jax.ShapeDtypeStruct((v_own, rows), bf),
        ]
        parts = pl.pallas_call(
            functools.partial(kernel, n2, n1, pack),
            out_shape=results,
            in_specs=[hbm] * 8,
            out_specs=[hbm] * 4,
            scratch_shapes=[
                pltpu.VMEM((chunks, ROWS, d_model), bf),
                pltpu.VMEM((thirds, 2 * ff_own // thirds, d_model), bf),
                pltpu.VMEM((ff_tp, d_local), bf),
                pltpu.VMEM((v_tp, d_local), bf),
                pltpu.VMEM((chunks, ff_tp, ROWS), bf),
                pltpu.VMEM((chunks, 2, ROWS, half), bf),
                pltpu.VMEM((chunks, ROWS, half), bf),
                pltpu.VMEM((chunks, ROWS, half), bf),
                pltpu.VMEM((chunks, n_x - 1, blk, half), bf),
                pltpu.VMEM((chunks, 2, ROWS, half), bf),
                pltpu.VMEM((chunks, n2, 8, ROWS), f32),
                pltpu.VMEM((chunks, ROWS, d_local), bf),
                pltpu.VMEM((chunks, n2, window, ROWS), f32),
                pltpu.VMEM((chunks, 2, part, ROWS), f32),
                pltpu.VMEM((chunks, 2, part, ROWS), f32),
                pltpu.VMEM((chunks, 2, part, ROWS), f32),
                pltpu.VMEM((ROWS, LANES), f32),
                pltpu.VMEM((n2 * n1, 8, ROWS), f32),
                pltpu.VMEM((n1, 4, 1, rows - ROWS), f32),
                pltpu.VMEM((n2, 4, 1, rows - ROWS), f32),
                pltpu.VMEM((n2 * n1, 4, 1, ROWS), f32),
                pltpu.VMEM((1, d_model), f32),
                pltpu.VMEM((1, rows), f32),
                pltpu.VMEM((1, rows), jnp.int32),
                pltpu.VMEM((1, rows), f32),
                pltpu.VMEM((1, rows), f32),
                pltpu.VMEM((1, rows), f32),
                pltpu.VMEM((v_own, rows), bf),
                pltpu.SemaphoreType.DMA((n_loads,)),
                pltpu.SemaphoreType.DMA((n_copies,)),
                pltpu.SemaphoreType.DMA((n_copies,)),
                pltpu.SemaphoreType.DMA((2, 2)),
            ],
            compiler_params=pltpu.CompilerParams(
                collective_id=0, has_side_effects=True, vmem_limit_bytes=66_000_000,
            ),
            name="decode_tail",
        )(
            hidden, w_gate.T, w_up.T, w_down, row(norm_gain), w_vocab.T,
            row(temperature), row(target),
        )
        ln, ent, tgt, lp = pl.pallas_call(
            emit, out_shape=results, in_specs=[hbm] * 4, out_specs=[hbm] * 4,
            scratch_shapes=[pltpu.VMEM(r.shape, r.dtype) for r in results]
            + [pltpu.SemaphoreType.DMA((2, 7))],
            name="emit",
        )(*parts)
        return ln.reshape(rows), ent.reshape(rows), tgt.reshape(rows), lp.T

    return jax.shard_map(
        device_step, mesh=mesh,
        in_specs=(
            P("dp", None), P(None, ("tp", "tp2")), P(None, ("tp", "tp2")), P("tp", "tp2"),
            P(None), P("tp2", "tp"), P("dp"), P("dp"),
        ),
        out_specs=(P("dp"), P("dp"), P("dp"), P("dp", ("tp", "tp2"))),
        check_vma=False,
    )
```

```python
import functools

import jax
import jax.numpy as jnp
from jax import lax
from jax.experimental import pallas as pl
from jax.experimental.pallas import tpu as pltpu
from jax.sharding import PartitionSpec as P

NORM_EPS = 1e-6
ROWS = 128
LANES = 128
MESH = pl.DeviceIdType.MESH


class Sems:
    def __init__(self, ref):
        self.ref, self.used = ref, 0

    def take(self):
        self.used += 1
        return self.ref.at[self.used - 1]


def kernel(
    n2, n1, pack,
    hidden, w_gate, w_up, w_down, gain_in, w_vocab, temp_in, target_in,
    out_ln, out_ent, out_tgt, out_lp,
    hid, wgu, wd, wv, act_t, yp, pair, chip, xr, ys, sq, xs,
    lg, far, mrg, dct, sq_col, sq_all, st_a, st_y, st_b, gain, temp, target, ln, ent, tgt_lp, lp_out,
    load_sems, send_sems, recv_sems, cast_sems,
):
    chunks, _, d_model = hid.shape
    thirds, ff_part = wgu.shape[0], wgu.shape[1] // 2
    ff_own = thirds * ff_part
    d_local = wd.shape[1]
    half = d_local // 2
    v_own = out_lp.shape[0]
    n_x = n1 // 2
    blk = ROWS // n_x
    y = lax.axis_index("tp2")
    tp = lax.axis_index("tp")
    x, core = tp // 2, tp % 2
    loads = Sems(load_sems)
    send_ids, recv_ids = {}, {}

    def at_y(j):
        return {"tp2": (y + j) % n2}

    def at_x(j):
        return {"tp": ((x + j) % n_x) * 2 + core}

    partner = {"tp": x * 2 + (1 - core)}

    def remote(src, dst, device, out, into):
        return pltpu.make_async_remote_copy(
            src_ref=src, dst_ref=dst,
            send_sem=send_sems.at[send_ids.setdefault(out, len(send_ids))],
            recv_sem=recv_sems.at[recv_ids.setdefault(into, len(recv_ids))],
            device_id=device, device_id_type=MESH,
        )

    def send(copy):
        copy.start()

    def arrived(into, amount):
        pltpu.make_async_copy(amount, amount, recv_sems.at[recv_ids[into]]).wait()

    everyone = sorted(
        [(j2, j1) for j2 in range(n2) for j1 in range(n1)][1:],
        key=lambda j: -min(j[0], n2 - j[0]) - min(j[1] // 2, n_x - j[1] // 2),
    )

    def slot_of(y_from, tp_from):
        return ((y + n2 - y_from) % n2) * n1 + (tp + n1 - tp_from) % n1

    def broadcast(buf, index):
        for j2, j1 in everyone:
            pltpu.make_async_remote_copy(
                src_ref=buf.at[0], dst_ref=buf.at[j2 * n1 + j1],
                send_sem=cast_sems.at[index, 0], recv_sem=cast_sems.at[index, 1],
                device_id={"tp2": (y + j2) % n2, "tp": (tp + j1) % n1}, device_id_type=MESH,
            ).start()

    def wait_cast(buf, index, side):
        rest = buf.at[pl.ds(1, n2 * n1 - 1)]
        pltpu.make_async_copy(rest, rest, cast_sems.at[index, side]).wait()

    ff_cut = (ff_own // 2) // 16 * 16
    v_cut = (v_own // 2) // 8 * 8

    def act_rows(i, q, lo, size):
        return act_t.at[i, pl.ds(pl.multiple_of(q * ff_own + lo, 16), size), :]

    def q_of(slot):
        return (y + slot) % n2

    def base_of(slot):
        return pl.multiple_of((v_own * q_of(slot)) // 16 * 16, 16)

    def off_of(slot):
        return pl.multiple_of((v_own * q_of(slot)) % 16, 8)

    def lg_part(i, slot, part):
        lo, size = (0, v_cut) if part == 0 else (v_cut, v_own - v_cut)
        return lg.at[i, slot, pl.ds(pl.multiple_of(off_of(slot) + lo, 8), size), :]

    def part_of(buf, i, part):
        return buf.at[i, part, pl.ds(0, v_cut if part == 0 else v_own - v_cut), :]

    def pieces(i, slot, part, buf):
        lo, size = (0, v_cut) if part == 0 else (v_cut, v_own - v_cut)
        cut = size // 2 // 8 * 8 if i == 0 else size
        for at, n in ((0, cut), (cut, size - cut)):
            if n > 0:
                src = pl.ds(pl.multiple_of(off_of(slot) + lo + at, 8), n)
                yield lg.at[i, slot, src, :], buf.at[i, part, pl.ds(at, n), :]

    x_order = [n_x // 2] + [j for j in range(1, n_x) if j != n_x // 2]

    cps = []
    for i in range(chunks):
        c = {}
        parts = thirds if i == 0 else 1
        own = [act_rows(i, y, t * (ff_own // parts), ff_own // parts) for t in range(parts)]
        up, dn = ("act", "act") if i == 0 else ("up", "dn")
        c["own_up"] = [remote(a, a, at_y(1), "act", (up, i)) for a in own]
        c["own_dn"] = [remote(a, a, at_y(-1), "act", (dn, i)) for a in own]
        prev, nxt = (y + n2 - 1) % n2, (y + 1) % n2
        if i == 0:
            c["own_far"] = [remote(a, a, at_y(2), "act", (up, i)) for a in own]
        else:
            lo_half = act_rows(i, prev, 0, ff_cut)
            hi_half = act_rows(i, nxt, ff_cut, ff_own - ff_cut)
            c["fwd_up"] = remote(lo_half, lo_half, at_y(1), "act", ("fwd", i))
            c["fwd_dn"] = remote(hi_half, hi_half, at_y(-1), "act", ("fwd", i))
        c["pair"] = remote(yp.at[i, 1 - core], pair.at[i], partner, "pair", ("pair", i))
        c["xrs"] = [
            remote(
                chip.at[i, pl.ds(pl.multiple_of(((x + j) % n_x) * blk, blk), blk), :],
                xr.at[i, j - 1], at_x(j), "xrs", ("xrs", i),
            )
            for j in x_order
        ]
        mine = ys.at[i, core, pl.ds(pl.multiple_of(x * blk, blk), blk), :]
        c["xag"] = [remote(mine, mine, at_x(j), "xag", ("xag", i)) for j in x_order]
        c["swap"] = remote(ys.at[i, core], ys.at[i, core], partner, "swap", ("swap", i))
        c["ssq"] = [] if i == 0 else [
            remote(sq.at[i, 0], sq.at[i, j], at_y(j), "ssq", ("ssq", i)) for j in range(1, n2)
        ]
        for name, slot, part, buf, way in (
            ("far_a", 2, 0, far, -1), ("far_b", 2, 1, far, 1),
            ("mrg_a", 3, 0, mrg, -1), ("mrg_b", 1, 1, mrg, 1),
        ):
            into = name if buf is far else "mrg"
            c[name] = remote(lg_part(i, slot, part), part_of(buf, i, part), at_y(way), "lg", (into, i))
        for name, slot, part, way in (("dir_a", 1, 0, 1), ("dir_b", 3, 1, -1)):
            c[name] = [remote(a, b, at_y(way), "lg", ("dir", i)) for a, b in pieces(i, slot, part, dct)]
        cps.append(c)
    cp_tp = [
        remote(st_a.at[0], st_a.at[j], {"tp": (tp + j) % n1}, "tp", "tp") for j in range(n1 - 1, 0, -1)
    ]
    cp_y = [remote(st_y.at[0], st_y.at[j], at_y(j), "y", "y") for j in range(1, n2)]
    all_sent = {
        "act": act_t.at[:, pl.ds(0, (n2 - 1) * ff_own), :], "pair": pair, "xrs": xr, "xag": xr, "swap": pair,
        "ssq": sq.at[pl.ds(1, chunks - 1), pl.ds(1, n2 - 1)],
        "lg": lg.at[:, pl.ds(0, 3), pl.ds(0, v_own), :],
        "tp": st_a.at[pl.ds(1, n1 - 1)], "y": st_y.at[pl.ds(1, n2 - 1)],
    }

    def load(src, dst):
        return pltpu.make_async_copy(src, dst, loads.take())

    def load_rows(src, dst, parts):
        rows, sem = src[0].shape[0] // parts, loads.take()
        cps = [
            pltpu.make_async_copy(a.at[pl.ds(k * rows, rows)], b.at[pl.ds(k * rows, rows)], sem)
            for k in range(parts) for a, b in zip(src, dst)
        ]
        return cps, sem

    ld_hid = [
        load_rows(
            [hidden.at[pl.ds(j * ROWS, ROWS), :] for j in range(i, i + pack)],
            [hid.at[j] for j in range(i, i + pack)], 2,
        )
        for i in range(0, chunks, pack)
    ]
    ld_w = [
        load_rows(
            [w.at[pl.ds(t * ff_part, ff_part), :] for w in (w_gate, w_up)],
            [wgu.at[t, pl.ds(side * ff_part, ff_part), :] for side in range(2)],
            3 if ff_part % 48 == 0 else 1,
        )
        for t in range(thirds)
    ]

    def wait_load(group, dst):
        pltpu.make_async_copy(dst, dst, group[1]).wait()

    ld_wd = load(w_down, wd)
    ld_wv = load(w_vocab, wv)
    ld_small = [load(gain_in, gain), load(temp_in, temp), load(target_in, target)]
    peers = [{"tp2": (y + j2) % n2, "tp": (tp + j1) % n1} for j2, j1 in everyone]
    with jax.named_scope("start"):
        for cp in [cp for group in [ld_hid[0]] + ld_w for cp in group[0]]:
            cp.start()
        for cp in ld_small:
            cp.start()
        barrier = pltpu.get_barrier_semaphore()
        for device in peers:
            pl.semaphore_signal(barrier, inc=1, device_id=device, device_id_type=MESH)

    NT = (((1,), (1,)), ((), ()))

    def gate_up(first, t):
        r = lax.dot_general(
            wgu[t], hid[first:first + pack].reshape(pack * ROWS, d_model), NT,
            preferred_element_type=jnp.float32,
        )
        act = (jax.nn.silu(r[:ff_part]) * r[ff_part:]).astype(jnp.bfloat16)
        for i in range(pack):
            at = pl.ds(pl.multiple_of(y * ff_own + t * ff_part, 16), ff_part)
            act_t[first + i, at, :] = act[:, i * ROWS:(i + 1) * ROWS]

    def send_own(i, t=0):
        send(cps[i]["own_up"][t])
        if i == 0:
            send(cps[i]["own_far"][t])
        send(cps[i]["own_dn"][t])

    def forward(i):
        amount = act_t.at[i, pl.ds(0, ff_own), :]
        arrived(("up", i), amount)
        send(cps[i]["fwd_up"])
        arrived(("dn", i), amount)
        send(cps[i]["fwd_dn"])

    def down(i):
        name, count = ("act", n2 - 1) if i == 0 else ("fwd", 1)
        arrived((name, i), act_t.at[i, pl.ds(0, count * ff_own), :])
        if i == 0:
            ld_wd.wait()
        for s in range(2):
            yp[i, s] = lax.dot_general(
                act_t[i], wd[:, s * half:(s + 1) * half],
                (((0,), (0,)), ((), ())), preferred_element_type=jnp.float32,
            ).astype(jnp.bfloat16)
        send(cps[i]["pair"])

    def chip_sum(i):
        arrived(("pair", i), pair.at[i])
        chip[i] = (
            yp[i, core].astype(jnp.float32) + pair[i].astype(jnp.float32)
        ).astype(jnp.bfloat16)
        for cp in cps[i]["xrs"]:
            send(cp)

    def row_sum(i):
        at = pl.ds(pl.multiple_of(x * blk, blk), blk)
        total = chip[i, at, :].astype(jnp.float32)
        arrived(("xrs", i), xr.at[i])
        for j in x_order:
            total += xr[i, j - 1].astype(jnp.float32)
        total = total.astype(jnp.bfloat16)
        ys[i, core, at, :] = total
        for cp in cps[i]["xag"]:
            send(cp)
        if i == 0:
            cols = pl.ds(pl.multiple_of(y * d_local + core * half, LANES), half)
            r = hid[i, at, cols].astype(jnp.float32) + total.astype(jnp.float32)
            part = jnp.sum(r * r, axis=1, keepdims=True)
            sq_col[...] = jnp.zeros_like(sq_col)
            sq_col[at, :] = jnp.broadcast_to(part, (blk, LANES))
            sq_all[0] = sq_col[...].T[:8, :]
            broadcast(sq_all, 0)

    def swap(i):
        arrived(("xag", i), xr.at[i])
        send(cps[i]["swap"])

    def residual(i, s):
        cols = pl.ds(pl.multiple_of(y * d_local + s * half, LANES), half)
        return hid[i, :, cols].astype(jnp.float32) + ys[i, s].astype(jnp.float32)

    def square(i):
        arrived(("swap", i), pair.at[i])
        part = 0.0
        for s in range(2):
            r = residual(i, s)
            part = part + jnp.sum(r * r, axis=1, keepdims=True)
        sq[i, 0] = jnp.broadcast_to(part, (ROWS, LANES)).T[:8, :]
        for cp in cps[i]["ssq"]:
            send(cp)

    def norm(i):
        if i == 0:
            arrived(("swap", i), pair.at[i])
            wait_cast(sq_all, 0, 1)
            total = jnp.sum(sq_all[...], axis=0)
        else:
            total = sq[i, 0]
            arrived(("ssq", i), sq.at[i, pl.ds(1, n2 - 1)])
            for j in range(1, n2):
                total = total + sq[i, j]
        inv = lax.rsqrt(total / d_model + NORM_EPS)
        inv = jnp.broadcast_to(inv[:1, :], (LANES, ROWS)).T[:, :1]
        for s in range(2):
            g = gain[:, pl.ds(pl.multiple_of(y * d_local + s * half, LANES), half)]
            xs[i, :, s * half:(s + 1) * half] = (g * residual(i, s) * inv).astype(jnp.bfloat16)

    window = lg.shape[2]
    step = window // 3 if window % 48 == 0 else window

    def piece(i, slot, at, size):
        lg[i, slot, pl.ds(at, size), :] = lax.dot_general(
            wv[pl.ds(pl.multiple_of(base_of(slot) + at, 16), size), :], xs[i], NT,
            preferred_element_type=jnp.float32,
        )

    def logits(i, slot):
        @pl.loop(0, window // step)
        def _(j):
            piece(i, slot, pl.multiple_of(j * step, 16), step)

    def logits_far(i):
        if i == 0:
            cut = -(-(v_cut + 8) // 16) * 16
            piece(i, 2, 0, cut)
            send(cps[i]["far_a"])
            piece(i, 2, cut, window - cut)
        else:
            logits(i, 2)
            send(cps[i]["far_a"])
        send(cps[i]["far_b"])

    def logits_up(i):
        logits(i, 1)
        send(cps[i]["dir_a"][0])

    def logits_down(i):
        logits(i, 3)
        send(cps[i]["dir_b"][0])

    def near_send(i):
        send(cps[i]["dir_a"][1])
        send(cps[i]["dir_b"][1])

    def merge(i):
        for name, slot, part in (("a", 3, 0), ("b", 1, 1)):
            arrived(("far_" + name, i), part_of(far, i, part))
            lg_part(i, slot, part)[...] += part_of(far, i, part)[...]
            send(cps[i]["mrg_" + name])

    def own(i):
        logits(i, 0)

    def near_sum(i):
        arrived(("dir", i), lg.at[i, 0, pl.ds(0, v_own), :])
        for part in range(2):
            lg_part(i, 0, part)[...] += part_of(dct, i, part)[...]

    def finish(i):
        lanes = pl.ds(i * ROWS, ROWS)
        t = temp[:, lanes]
        tgt = target[:, lanes]
        col0 = (tp * n2 + y) * v_own
        peak = None
        arrived(("mrg", i), lg.at[i, 0, pl.ds(0, v_own), :])
        for part in range(2):
            ref = lg_part(i, 0, part)
            val = (ref[...] + part_of(mrg, i, part)[...]) / t
            ref[...] = val
            top = jnp.max(val, axis=0, keepdims=True)
            peak = top if peak is None else jnp.maximum(peak, top)
        total = dot = hit = 0.0
        for part in range(2):
            val = lg_part(i, 0, part)[...]
            e = jnp.exp(val - peak)
            total = total + jnp.sum(e, axis=0, keepdims=True)
            dot = dot + jnp.sum(e * val, axis=0, keepdims=True)
            ids = col0 + part * v_cut + lax.broadcasted_iota(jnp.int32, val.shape, 0)
            hit = hit + jnp.sum(jnp.where(ids == tgt, val, 0.0), axis=0, keepdims=True)
        buf, at = (st_b, slice(0, ROWS)) if i == chunks - 1 else (st_a, lanes)
        for row, v in enumerate((peak, total, dot, hit)):
            buf[0, row, :, at] = v

    def combine(buf, slots):
        peak = jnp.max(buf[:, 0], axis=0)
        total = dot = hit = 0.0
        for slot in slots:
            v = buf[slot]
            scale = jnp.exp(v[0] - peak)
            total = total + v[1] * scale
            dot = dot + v[2] * scale
            hit = hit + v[3]
        return peak, total, dot, hit

    def row_results(stats, lanes):
        peak, total, dot, hit = stats
        log_norm = peak + jnp.log(total)
        ln[:, lanes] = log_norm
        ent[:, lanes] = log_norm - dot / total
        tgt_lp[:, lanes] = hit - log_norm

    def output(first, count):
        for i in range(first, first + count):
            lanes = slice(i * ROWS, (i + 1) * ROWS)
            val = lg[i, 0, pl.ds(off_of(0), v_own), :]
            lp_out[:, lanes] = (val - ln[:, lanes]).astype(jnp.bfloat16)

    last = chunks - 1

    def run(*items):
        for fn, i in items:
            if 0 <= i <= last:
                with jax.named_scope(f"{fn.__name__}#c={i}"):
                    fn(i)

    wait_load(ld_hid[0], hid.at[pl.ds(0, pack)])
    for t in range(thirds):
        with jax.named_scope(f"gate_up#c=0#t={t}"):
            wait_load(ld_w[t], wgu.at[t])
            if t == thirds - 1:
                for cp in [cp for group in ld_hid[1:] for cp in group[0]]:
                    cp.start()
            gate_up(0, t)
        if t == 0:
            with jax.named_scope("barrier"):
                pl.semaphore_wait(barrier, len(peers))
        send_own(0, t)
    ld_wd.start()
    for i in range(1, pack):
        send_own(i)
    ld_wv.start()
    for i in range(pack, chunks, pack):
        wait_load(ld_hid[i // pack], hid.at[pl.ds(i, pack)])
        with jax.named_scope(f"gate_up#c={i}"):
            for t in range(thirds):
                gate_up(i, t)
    for cp in ld_small:
        cp.wait()
    run((send_own, 2), (down, 0), (chip_sum, 0), (forward, 1), (row_sum, 0), (send_own, 3))
    run((forward, 2), (down, 1), (swap, 0), (chip_sum, 1), (norm, 0), (forward, 3))
    ld_wv.wait()
    run((logits_far, 0), (logits_up, 0), (row_sum, 1), (logits_down, 0), (down, 2), (down, 3), (chip_sum, 2))
    run((chip_sum, 3), (swap, 1), (square, 1), (near_send, 0), (row_sum, 2), (norm, 1))
    run((logits_far, 1), (row_sum, 3), (swap, 2), (square, 2), (merge, 0), (logits_up, 1), (logits_down, 1))
    run((swap, 3), (square, 3), (norm, 2))
    for i in range(1, chunks - 1):
        run((logits_far, i + 1), (merge, i), (logits_up, i + 1), (logits_down, i + 1), (norm, i + 2))
        run((own, i - 1), (near_sum, i - 1))
    run((finish, last - 3), (own, last - 1), (own, last), (near_sum, last - 1), (finish, last - 2))
    run((merge, last), (finish, last - 1))
    for cp in cp_tp:
        send(cp)
    run((near_sum, last),)
    with jax.named_scope("stats_tp"):
        arrived("tp", st_a.at[pl.ds(1, n1 - 1)])
        for row, v in enumerate(combine(st_a, [(tp + n1 - j) % n1 for j in range(n1)])):
            st_y[0, row] = v
        for cp in cp_y:
            send(cp)
    run((finish, last),)
    with jax.named_scope("cast_b"):
        broadcast(st_b, 1)
    with jax.named_scope("output_a"):
        arrived("y", st_y.at[pl.ds(1, n2 - 1)])
        row_results(combine(st_y, [(y + n2 - j) % n2 for j in range(n2)]), slice(0, last * ROWS))
        output(0, last)
        first_store = load(lp_out.at[:, :last * ROWS], out_lp.at[:, :last * ROWS])
        first_store.start()
    with jax.named_scope("sent"):
        for out, amount in all_sent.items():
            pltpu.make_async_copy(amount, amount, send_sems.at[send_ids[out]]).wait()
        wait_cast(sq_all, 0, 0)
    with jax.named_scope("wait_b"):
        wait_cast(st_b, 1, 1)
    with jax.named_scope("output_b"):
        order = [slot_of(j2, j1) for j2 in range(n2) for j1 in range(n1)]
        row_results(combine(st_b, order), slice(last * ROWS, chunks * ROWS))
        output(last, 1)
    with jax.named_scope("drain"):
        stores = [load(lp_out.at[:, last * ROWS:], out_lp.at[:, last * ROWS:])]
        stores += [load(a, b) for a, b in ((ln, out_ln), (ent, out_ent), (tgt_lp, out_tgt))]
        for cp in stores:
            cp.start()
        wait_cast(st_b, 1, 0)
        for cp in [first_store] + stores:
            cp.wait()


def emit(*refs):
    ins, outs, bufs, sems = refs[:4], refs[4:8], refs[8:12], refs[12]
    rows = ins[3].shape[0]
    cut = -(-rows // 64) * 16
    pieces = [(3, pl.ds(lo, min(cut, rows - lo))) for lo in range(0, rows, cut)]
    pieces += [(n, pl.ds(0, 1)) for n in range(3)]
    taken = [
        pltpu.make_async_copy(ins[n].at[at, :], bufs[n].at[at, :], sems.at[0, k])
        for k, (n, at) in enumerate(pieces)
    ]
    given = [
        pltpu.make_async_copy(bufs[n].at[at, :], outs[n].at[at, :], sems.at[1, k])
        for k, (n, at) in enumerate(pieces)
    ]
    for cp in taken:
        cp.start()
    for a, b in zip(taken, given):
        a.wait()
        b.start()
    for cp in given:
        cp.wait()


def solution(mesh):
    n2, n1 = mesh.shape["tp2"], mesh.shape["tp"]

    def device_step(hidden, w_gate, w_up, w_down, norm_gain, w_vocab, temperature, target):
        rows, d_model = hidden.shape
        ff_own = w_gate.shape[1]
        ff_tp, d_local = w_down.shape
        v_tp = w_vocab.shape[1]
        v_own = v_tp // n2
        chunks = rows // ROWS
        half = d_local // 2
        n_x = n1 // 2
        blk = ROWS // n_x
        pack = min(2, chunks)
        thirds = 3 if ff_own % 48 == 0 else 1
        window = -(-v_own // 16) * 16
        part = v_own - (v_own // 2) // 8 * 8
        bf, f32 = jnp.bfloat16, jnp.float32
        n_loads = -(-chunks // pack) + thirds + 2 + 3 + 5
        n_arrivals = 9 + 12 * (chunks - 1) + 2
        row = lambda a: a.reshape(1, -1)
        vmem = pl.BlockSpec(memory_space=pltpu.VMEM)
        hbm = pl.BlockSpec(memory_space=pl.ANY)
        results = [
            jax.ShapeDtypeStruct((1, rows), f32),
            jax.ShapeDtypeStruct((1, rows), f32),
            jax.ShapeDtypeStruct((1, rows), f32),
            jax.ShapeDtypeStruct((v_own, rows), bf),
        ]
        parts = pl.pallas_call(
            functools.partial(kernel, n2, n1, pack),
            out_shape=results,
            in_specs=[hbm] * 8,
            out_specs=[hbm] * 4,
            scratch_shapes=[
                pltpu.VMEM((chunks, ROWS, d_model), bf),
                pltpu.VMEM((thirds, 2 * ff_own // thirds, d_model), bf),
                pltpu.VMEM((ff_tp, d_local), bf),
                pltpu.VMEM((v_tp, d_local), bf),
                pltpu.VMEM((chunks, ff_tp, ROWS), bf),
                pltpu.VMEM((chunks, 2, ROWS, half), bf),
                pltpu.VMEM((chunks, ROWS, half), bf),
                pltpu.VMEM((chunks, ROWS, half), bf),
                pltpu.VMEM((chunks, n_x - 1, blk, half), bf),
                pltpu.VMEM((chunks, 2, ROWS, half), bf),
                pltpu.VMEM((chunks, n2, 8, ROWS), f32),
                pltpu.VMEM((chunks, ROWS, d_local), bf),
                pltpu.VMEM((chunks, n2, window, ROWS), f32),
                pltpu.VMEM((chunks, 2, part, ROWS), f32),
                pltpu.VMEM((chunks, 2, part, ROWS), f32),
                pltpu.VMEM((chunks, 2, part, ROWS), f32),
                pltpu.VMEM((ROWS, LANES), f32),
                pltpu.VMEM((n2 * n1, 8, ROWS), f32),
                pltpu.VMEM((n1, 4, 1, rows - ROWS), f32),
                pltpu.VMEM((n2, 4, 1, rows - ROWS), f32),
                pltpu.VMEM((n2 * n1, 4, 1, ROWS), f32),
                pltpu.VMEM((1, d_model), f32),
                pltpu.VMEM((1, rows), f32),
                pltpu.VMEM((1, rows), jnp.int32),
                pltpu.VMEM((1, rows), f32),
                pltpu.VMEM((1, rows), f32),
                pltpu.VMEM((1, rows), f32),
                pltpu.VMEM((v_own, rows), bf),
                pltpu.SemaphoreType.DMA((n_loads,)),
                pltpu.SemaphoreType.DMA((9,)),
                pltpu.SemaphoreType.DMA((n_arrivals,)),
                pltpu.SemaphoreType.DMA((2, 2)),
            ],
            compiler_params=pltpu.CompilerParams(
                collective_id=0, has_side_effects=True, vmem_limit_bytes=66_000_000,
            ),
            name="decode_tail",
        )(
            hidden, w_gate.T, w_up.T, w_down, row(norm_gain), w_vocab.T,
            row(temperature), row(target),
        )
        ln, ent, tgt, lp = pl.pallas_call(
            emit, out_shape=results, in_specs=[hbm] * 4, out_specs=[hbm] * 4,
            scratch_shapes=[pltpu.VMEM(r.shape, r.dtype) for r in results]
            + [pltpu.SemaphoreType.DMA((2, 7))],
            name="emit",
        )(*parts)
        return ln.reshape(rows), ent.reshape(rows), tgt.reshape(rows), lp.T

    return jax.shard_map(
        device_step, mesh=mesh,
        in_specs=(
            P("dp", None), P(None, ("tp", "tp2")), P(None, ("tp", "tp2")), P("tp", "tp2"),
            P(None), P("tp2", "tp"), P("dp"), P("dp"),
        ),
        out_specs=(P("dp"), P("dp"), P("dp"), P("dp", ("tp", "tp2"))),
        check_vma=False,
    )
```

```python
import functools

import jax
import jax.numpy as jnp
from jax import lax
from jax.experimental import pallas as pl
from jax.experimental.pallas import tpu as pltpu
from jax.sharding import PartitionSpec as P

NORM_EPS = 1e-6
ROWS = 128
LANES = 128
MESH = pl.DeviceIdType.MESH


class Sems:
    def __init__(self, ref):
        self.ref, self.used = ref, 0

    def take(self):
        self.used += 1
        return self.ref.at[self.used - 1]


def kernel(
    n2, n1, pack,
    hidden, w_gate, w_up, w_down, gain_in, w_vocab, temp_in, target_in,
    out_ln, out_ent, out_tgt, out_lp,
    hid, wgu, wd, wv, act_t, yp, pair, chip, xr, ys, sq, xs,
    lg, far, mrg, dct, sq_col, sq_all, st_a, st_y, st_b, gain, temp, target, ln, ent, tgt_lp, lp_out,
    load_sems, send_sems, recv_sems, cast_sems,
):
    chunks, _, d_model = hid.shape
    thirds, ff_part = wgu.shape[0], wgu.shape[1] // 2
    ff_own = thirds * ff_part
    d_local = wd.shape[1]
    half = d_local // 2
    v_own = out_lp.shape[0]
    n_x = n1 // 2
    blk = ROWS // n_x
    y = lax.axis_index("tp2")
    tp = lax.axis_index("tp")
    x, core = tp // 2, tp % 2
    loads = Sems(load_sems)
    send_ids, recv_ids = {}, {}

    def at_y(j):
        return {"tp2": (y + j) % n2}

    def at_x(j):
        return {"tp": ((x + j) % n_x) * 2 + core}

    partner = {"tp": x * 2 + (1 - core)}

    def remote(src, dst, device, out, into):
        return pltpu.make_async_remote_copy(
            src_ref=src, dst_ref=dst,
            send_sem=send_sems.at[send_ids.setdefault(out, len(send_ids))],
            recv_sem=recv_sems.at[recv_ids.setdefault(into, len(recv_ids))],
            device_id=device, device_id_type=MESH,
        )

    def send(copy):
        copy.start()

    def arrived(into, amount):
        pltpu.make_async_copy(amount, amount, recv_sems.at[recv_ids[into]]).wait()

    everyone = sorted(
        [(j2, j1) for j2 in range(n2) for j1 in range(n1)][1:],
        key=lambda j: -min(j[0], n2 - j[0]) - min(j[1] // 2, n_x - j[1] // 2),
    )

    def slot_of(y_from, tp_from):
        return ((y + n2 - y_from) % n2) * n1 + (tp + n1 - tp_from) % n1

    def broadcast(buf, index):
        for j2, j1 in everyone:
            pltpu.make_async_remote_copy(
                src_ref=buf.at[0], dst_ref=buf.at[j2 * n1 + j1],
                send_sem=cast_sems.at[index, 0], recv_sem=cast_sems.at[index, 1],
                device_id={"tp2": (y + j2) % n2, "tp": (tp + j1) % n1}, device_id_type=MESH,
            ).start()

    def wait_cast(buf, index, side):
        rest = buf.at[pl.ds(1, n2 * n1 - 1)]
        pltpu.make_async_copy(rest, rest, cast_sems.at[index, side]).wait()

    ff_cut = (ff_own // 2) // 16 * 16
    v_cut = (v_own // 2) // 8 * 8

    def act_rows(i, q, lo, size):
        return act_t.at[i, pl.ds(pl.multiple_of(q * ff_own + lo, 16), size), :]

    def q_of(slot):
        return (y + slot) % n2

    def base_of(slot):
        return pl.multiple_of((v_own * q_of(slot)) // 16 * 16, 16)

    def off_of(slot):
        return pl.multiple_of((v_own * q_of(slot)) % 16, 8)

    def lg_part(i, slot, part):
        lo, size = (0, v_cut) if part == 0 else (v_cut, v_own - v_cut)
        return lg.at[i, slot, pl.ds(pl.multiple_of(off_of(slot) + lo, 8), size), :]

    def part_of(buf, i, part):
        return buf.at[i, part, pl.ds(0, v_cut if part == 0 else v_own - v_cut), :]

    def pieces(i, slot, part, buf):
        lo, size = (0, v_cut) if part == 0 else (v_cut, v_own - v_cut)
        cut = size // 2 // 8 * 8 if i == 0 else size
        for at, n in ((0, cut), (cut, size - cut)):
            if n > 0:
                src = pl.ds(pl.multiple_of(off_of(slot) + lo + at, 8), n)
                yield lg.at[i, slot, src, :], buf.at[i, part, pl.ds(at, n), :]

    x_order = [n_x // 2] + [j for j in range(1, n_x) if j != n_x // 2]

    cps = []
    for i in range(chunks):
        c = {}
        parts = thirds if i == 0 else 1
        own = [act_rows(i, y, t * (ff_own // parts), ff_own // parts) for t in range(parts)]
        up, dn = ("act", "act") if i == 0 else ("up", "dn")
        c["own_up"] = [remote(a, a, at_y(1), "act", (up, i)) for a in own]
        c["own_dn"] = [remote(a, a, at_y(-1), "act", (dn, i)) for a in own]
        prev, nxt = (y + n2 - 1) % n2, (y + 1) % n2
        if i == 0:
            c["own_far"] = [remote(a, a, at_y(2), "act", (up, i)) for a in own]
        else:
            lo_half = act_rows(i, prev, 0, ff_cut)
            hi_half = act_rows(i, nxt, ff_cut, ff_own - ff_cut)
            c["fwd_up"] = remote(lo_half, lo_half, at_y(1), "act", ("fwd", i))
            c["fwd_dn"] = remote(hi_half, hi_half, at_y(-1), "act", ("fwd", i))
        c["pair"] = remote(yp.at[i, 1 - core], pair.at[i], partner, "pair", ("pair", i))
        c["xrs"] = [
            remote(
                chip.at[i, pl.ds(pl.multiple_of(((x + j) % n_x) * blk, blk), blk), :],
                xr.at[i, j - 1], at_x(j), "xrs", ("xrs", i),
            )
            for j in x_order
        ]
        mine = ys.at[i, core, pl.ds(pl.multiple_of(x * blk, blk), blk), :]
        c["xag"] = [remote(mine, mine, at_x(j), "xag", ("xag", i)) for j in x_order]
        c["swap"] = remote(ys.at[i, core], ys.at[i, core], partner, "swap", ("swap", i))
        c["ssq"] = [] if i == 0 else [
            remote(sq.at[i, 0], sq.at[i, j], at_y(j), "ssq", ("ssq", i)) for j in range(1, n2)
        ]
        for name, slot, part, buf, way in (
            ("far_a", 2, 0, far, -1), ("far_b", 2, 1, far, 1),
            ("mrg_a", 3, 0, mrg, -1), ("mrg_b", 1, 1, mrg, 1),
        ):
            into = name if buf is far else "mrg"
            c[name] = remote(lg_part(i, slot, part), part_of(buf, i, part), at_y(way), "lg", (into, i))
        for name, slot, part, way in (("dir_a", 1, 0, 1), ("dir_b", 3, 1, -1)):
            c[name] = [remote(a, b, at_y(way), "lg", ("dir", i)) for a, b in pieces(i, slot, part, dct)]
        cps.append(c)
    cp_tp = [
        remote(st_a.at[0], st_a.at[j], {"tp": (tp + j) % n1}, "tp", "tp") for j in range(n1 - 1, 0, -1)
    ]
    cp_y = [remote(st_y.at[0], st_y.at[j], at_y(j), "y", "y") for j in range(1, n2)]
    all_sent = {
        "act": act_t.at[:, pl.ds(0, (n2 - 1) * ff_own), :], "pair": pair, "xrs": xr, "xag": xr, "swap": pair,
        "ssq": sq.at[pl.ds(1, chunks - 1), pl.ds(1, n2 - 1)],
        "lg": lg.at[:, pl.ds(0, 3), pl.ds(0, v_own), :],
        "tp": st_a.at[pl.ds(1, n1 - 1)], "y": st_y.at[pl.ds(1, n2 - 1)],
    }

    def load(src, dst):
        return pltpu.make_async_copy(src, dst, loads.take())

    def load_rows(src, dst, parts):
        rows, sem = src[0].shape[0] // parts, loads.take()
        cps = [
            pltpu.make_async_copy(a.at[pl.ds(k * rows, rows)], b.at[pl.ds(k * rows, rows)], sem)
            for k in range(parts) for a, b in zip(src, dst)
        ]
        return cps, sem

    ld_hid = [
        load_rows(
            [hidden.at[pl.ds(j * ROWS, ROWS), :] for j in range(i, i + pack)],
            [hid.at[j] for j in range(i, i + pack)], 2,
        )
        for i in range(0, chunks, pack)
    ]
    ld_w = [
        load_rows(
            [w.at[pl.ds(t * ff_part, ff_part), :] for w in (w_gate, w_up)],
            [wgu.at[t, pl.ds(side * ff_part, ff_part), :] for side in range(2)],
            3 if ff_part % 48 == 0 else 1,
        )
        for t in range(thirds)
    ]

    def wait_load(group, dst):
        pltpu.make_async_copy(dst, dst, group[1]).wait()

    ld_wd = load(w_down, wd)
    ld_wv = load(w_vocab, wv)
    ld_small = [load(gain_in, gain), load(temp_in, temp), load(target_in, target)]
    peers = [{"tp2": (y + j2) % n2, "tp": (tp + j1) % n1} for j2, j1 in everyone]
    with jax.named_scope("start"):
        for cp in [cp for group in [ld_hid[0]] + ld_w for cp in group[0]]:
            cp.start()
        for cp in ld_small:
            cp.start()
        barrier = pltpu.get_barrier_semaphore()
        for device in peers:
            pl.semaphore_signal(barrier, inc=1, device_id=device, device_id_type=MESH)

    NT = (((1,), (1,)), ((), ()))

    def gate_up(first, at, count):
        r = lax.dot_general(
            wgu[at:at + count].reshape(count * 2 * ff_part, d_model),
            hid[first:first + pack].reshape(pack * ROWS, d_model), NT,
            preferred_element_type=jnp.float32,
        )
        for t in range(count):
            lo = t * 2 * ff_part
            g, u = r[lo:lo + ff_part], r[lo + ff_part:lo + 2 * ff_part]
            act = (jax.nn.silu(g) * u).astype(jnp.bfloat16)
            for i in range(pack):
                rows = pl.ds(pl.multiple_of(y * ff_own + (at + t) * ff_part, 16), ff_part)
                act_t[first + i, rows, :] = act[:, i * ROWS:(i + 1) * ROWS]

    def send_own(i, t=0):
        send(cps[i]["own_up"][t])
        if i == 0:
            send(cps[i]["own_far"][t])
        send(cps[i]["own_dn"][t])

    def forward(i):
        amount = act_t.at[i, pl.ds(0, ff_own), :]
        arrived(("up", i), amount)
        send(cps[i]["fwd_up"])
        arrived(("dn", i), amount)
        send(cps[i]["fwd_dn"])

    def down(i):
        name, count = ("act", n2 - 1) if i == 0 else ("fwd", 1)
        arrived((name, i), act_t.at[i, pl.ds(0, count * ff_own), :])
        if i == 0:
            ld_wd.wait()
        for s in range(2):
            yp[i, s] = lax.dot_general(
                act_t[i], wd[:, s * half:(s + 1) * half],
                (((0,), (0,)), ((), ())), preferred_element_type=jnp.float32,
            ).astype(jnp.bfloat16)
        send(cps[i]["pair"])

    def chip_sum(i):
        arrived(("pair", i), pair.at[i])
        chip[i] = (
            yp[i, core].astype(jnp.float32) + pair[i].astype(jnp.float32)
        ).astype(jnp.bfloat16)
        for cp in cps[i]["xrs"]:
            send(cp)

    def row_sum(i):
        at = pl.ds(pl.multiple_of(x * blk, blk), blk)
        total = chip[i, at, :].astype(jnp.float32)
        arrived(("xrs", i), xr.at[i])
        for j in x_order:
            total += xr[i, j - 1].astype(jnp.float32)
        total = total.astype(jnp.bfloat16)
        ys[i, core, at, :] = total
        for cp in cps[i]["xag"]:
            send(cp)
        if i == 0:
            cols = pl.ds(pl.multiple_of(y * d_local + core * half, LANES), half)
            r = hid[i, at, cols].astype(jnp.float32) + total.astype(jnp.float32)
            part = jnp.sum(r * r, axis=1, keepdims=True)
            sq_col[...] = jnp.zeros_like(sq_col)
            sq_col[at, :] = jnp.broadcast_to(part, (blk, LANES))
            sq_all[0] = sq_col[...].T[:8, :]
            broadcast(sq_all, 0)

    def swap(i):
        arrived(("xag", i), xr.at[i])
        send(cps[i]["swap"])

    def residual(i, s):
        cols = pl.ds(pl.multiple_of(y * d_local + s * half, LANES), half)
        return hid[i, :, cols].astype(jnp.float32) + ys[i, s].astype(jnp.float32)

    def square(i):
        arrived(("swap", i), pair.at[i])
        part = 0.0
        for s in range(2):
            r = residual(i, s)
            part = part + jnp.sum(r * r, axis=1, keepdims=True)
        sq[i, 0] = jnp.broadcast_to(part, (ROWS, LANES)).T[:8, :]
        for cp in cps[i]["ssq"]:
            send(cp)

    def norm(i):
        if i == 0:
            arrived(("swap", i), pair.at[i])
            wait_cast(sq_all, 0, 1)
            total = jnp.sum(sq_all[...], axis=0)
        else:
            total = sq[i, 0]
            arrived(("ssq", i), sq.at[i, pl.ds(1, n2 - 1)])
            for j in range(1, n2):
                total = total + sq[i, j]
        inv = lax.rsqrt(total / d_model + NORM_EPS)
        inv = jnp.broadcast_to(inv[:1, :], (LANES, ROWS)).T[:, :1]
        for s in range(2):
            g = gain[:, pl.ds(pl.multiple_of(y * d_local + s * half, LANES), half)]
            xs[i, :, s * half:(s + 1) * half] = (g * residual(i, s) * inv).astype(jnp.bfloat16)

    window = lg.shape[2]
    step = window // 3 if window % 48 == 0 else window

    def piece(i, slot, at, size):
        lg[i, slot, pl.ds(at, size), :] = lax.dot_general(
            wv[pl.ds(pl.multiple_of(base_of(slot) + at, 16), size), :], xs[i], NT,
            preferred_element_type=jnp.float32,
        )

    def logits(i, slot):
        @pl.loop(0, window // step)
        def _(j):
            piece(i, slot, pl.multiple_of(j * step, 16), step)

    def logits_far(i):
        if i == 0:
            cut = -(-(v_cut + 8) // 16) * 16
            piece(i, 2, 0, cut)
            send(cps[i]["far_a"])
            piece(i, 2, cut, window - cut)
        else:
            logits(i, 2)
            send(cps[i]["far_a"])
        send(cps[i]["far_b"])

    def logits_up(i):
        logits(i, 1)
        send(cps[i]["dir_a"][0])

    def logits_down(i):
        logits(i, 3)
        send(cps[i]["dir_b"][0])

    def near_send(i):
        send(cps[i]["dir_a"][1])
        send(cps[i]["dir_b"][1])

    def merge(i):
        for name, slot, part in (("a", 3, 0), ("b", 1, 1)):
            arrived(("far_" + name, i), part_of(far, i, part))
            lg_part(i, slot, part)[...] += part_of(far, i, part)[...]
            send(cps[i]["mrg_" + name])

    def own(i):
        logits(i, 0)

    def near_sum(i):
        arrived(("dir", i), lg.at[i, 0, pl.ds(0, v_own), :])
        for part in range(2):
            lg_part(i, 0, part)[...] += part_of(dct, i, part)[...]

    def finish(i):
        lanes = pl.ds(i * ROWS, ROWS)
        t = temp[:, lanes]
        tgt = target[:, lanes]
        col0 = (tp * n2 + y) * v_own
        peak = None
        arrived(("mrg", i), lg.at[i, 0, pl.ds(0, v_own), :])
        for part in range(2):
            ref = lg_part(i, 0, part)
            val = (ref[...] + part_of(mrg, i, part)[...]) / t
            ref[...] = val
            top = jnp.max(val, axis=0, keepdims=True)
            peak = top if peak is None else jnp.maximum(peak, top)
        total = dot = hit = 0.0
        for part in range(2):
            val = lg_part(i, 0, part)[...]
            e = jnp.exp(val - peak)
            total = total + jnp.sum(e, axis=0, keepdims=True)
            dot = dot + jnp.sum(e * val, axis=0, keepdims=True)
            ids = col0 + part * v_cut + lax.broadcasted_iota(jnp.int32, val.shape, 0)
            hit = hit + jnp.sum(jnp.where(ids == tgt, val, 0.0), axis=0, keepdims=True)
        buf, at = (st_b, slice(0, ROWS)) if i == chunks - 1 else (st_a, lanes)
        for row, v in enumerate((peak, total, dot, hit)):
            buf[0, row, :, at] = v

    def combine(buf, slots):
        peak = jnp.max(buf[:, 0], axis=0)
        total = dot = hit = 0.0
        for slot in slots:
            v = buf[slot]
            scale = jnp.exp(v[0] - peak)
            total = total + v[1] * scale
            dot = dot + v[2] * scale
            hit = hit + v[3]
        return peak, total, dot, hit

    def row_results(stats, lanes):
        peak, total, dot, hit = stats
        log_norm = peak + jnp.log(total)
        ln[:, lanes] = log_norm
        ent[:, lanes] = log_norm - dot / total
        tgt_lp[:, lanes] = hit - log_norm

    def output(first, count):
        for i in range(first, first + count):
            lanes = slice(i * ROWS, (i + 1) * ROWS)
            val = lg[i, 0, pl.ds(off_of(0), v_own), :]
            lp_out[:, lanes] = (val - ln[:, lanes]).astype(jnp.bfloat16)

    last = chunks - 1

    def run(*items):
        for fn, i in items:
            if 0 <= i <= last:
                with jax.named_scope(f"{fn.__name__}#c={i}"):
                    fn(i)

    wait_load(ld_hid[0], hid.at[pl.ds(0, pack)])
    wait_load(ld_w[0], wgu.at[0])
    gate_up(0, 0, 1)
    pl.semaphore_wait(barrier, len(peers))
    send_own(0, 0)
    if thirds > 1:
        wait_load(ld_w[1], wgu.at[1])
        wait_load(ld_w[2], wgu.at[2])
    for cp in [cp for group in ld_hid[1:] for cp in group[0]]:
        cp.start()
    if thirds > 1:
        gate_up(0, 1, 2)
        send_own(0, 1)
        send_own(0, 2)
    ld_wd.start()
    for i in range(1, pack):
        send_own(i)
    ld_wv.start()
    for i in range(pack, chunks, pack):
        wait_load(ld_hid[i // pack], hid.at[pl.ds(i, pack)])
        with jax.named_scope(f"gate_up#c={i}"):
            gate_up(i, 0, thirds)
    for cp in ld_small:
        cp.wait()
    run((send_own, 2), (down, 0), (chip_sum, 0), (forward, 1), (row_sum, 0), (send_own, 3))
    run((forward, 2), (down, 1), (swap, 0), (chip_sum, 1), (norm, 0), (forward, 3))
    ld_wv.wait()
    run((logits_far, 0), (logits_up, 0), (row_sum, 1), (logits_down, 0), (down, 2), (down, 3), (chip_sum, 2))
    run((chip_sum, 3), (swap, 1), (square, 1), (near_send, 0), (row_sum, 2), (norm, 1))
    run((logits_far, 1), (row_sum, 3), (swap, 2), (square, 2), (merge, 0), (logits_up, 1), (logits_down, 1))
    run((swap, 3), (square, 3), (norm, 2))
    for i in range(1, chunks - 1):
        run((logits_far, i + 1), (merge, i), (logits_up, i + 1), (logits_down, i + 1), (norm, i + 2))
        run((own, i - 1), (near_sum, i - 1))
    run((finish, last - 3), (own, last - 1), (own, last), (near_sum, last - 1), (finish, last - 2))
    run((merge, last), (finish, last - 1))
    for cp in cp_tp:
        send(cp)
    run((near_sum, last),)
    with jax.named_scope("stats_tp"):
        arrived("tp", st_a.at[pl.ds(1, n1 - 1)])
        for row, v in enumerate(combine(st_a, [(tp + n1 - j) % n1 for j in range(n1)])):
            st_y[0, row] = v
        for cp in cp_y:
            send(cp)
    run((finish, last),)
    with jax.named_scope("cast_b"):
        broadcast(st_b, 1)
    with jax.named_scope("output_a"):
        arrived("y", st_y.at[pl.ds(1, n2 - 1)])
        row_results(combine(st_y, [(y + n2 - j) % n2 for j in range(n2)]), slice(0, last * ROWS))
        output(0, last)
        first_store = load(lp_out.at[:, :last * ROWS], out_lp.at[:, :last * ROWS])
        first_store.start()
    with jax.named_scope("sent"):
        for out, amount in all_sent.items():
            pltpu.make_async_copy(amount, amount, send_sems.at[send_ids[out]]).wait()
        wait_cast(sq_all, 0, 0)
    with jax.named_scope("wait_b"):
        wait_cast(st_b, 1, 1)
    with jax.named_scope("output_b"):
        order = [slot_of(j2, j1) for j2 in range(n2) for j1 in range(n1)]
        row_results(combine(st_b, order), slice(last * ROWS, chunks * ROWS))
        output(last, 1)
    with jax.named_scope("drain"):
        stores = [load(lp_out.at[:, last * ROWS:], out_lp.at[:, last * ROWS:])]
        stores += [load(a, b) for a, b in ((ln, out_ln), (ent, out_ent), (tgt_lp, out_tgt))]
        for cp in stores:
            cp.start()
        wait_cast(st_b, 1, 0)
        for cp in [first_store] + stores:
            cp.wait()


def emit(*refs):
    ins, outs, bufs, sems = refs[:4], refs[4:8], refs[8:12], refs[12]
    rows = ins[3].shape[0]
    cut = -(-rows // 64) * 16
    pieces = [(3, pl.ds(lo, min(cut, rows - lo))) for lo in range(0, rows, cut)]
    pieces += [(n, pl.ds(0, 1)) for n in range(3)]
    taken = [
        pltpu.make_async_copy(ins[n].at[at, :], bufs[n].at[at, :], sems.at[0, k])
        for k, (n, at) in enumerate(pieces)
    ]
    given = [
        pltpu.make_async_copy(bufs[n].at[at, :], outs[n].at[at, :], sems.at[1, k])
        for k, (n, at) in enumerate(pieces)
    ]
    for cp in taken:
        cp.start()
    for a, b in zip(taken, given):
        a.wait()
        b.start()
    for cp in given:
        cp.wait()


def solution(mesh):
    n2, n1 = mesh.shape["tp2"], mesh.shape["tp"]

    def device_step(hidden, w_gate, w_up, w_down, norm_gain, w_vocab, temperature, target):
        rows, d_model = hidden.shape
        ff_own = w_gate.shape[1]
        ff_tp, d_local = w_down.shape
        v_tp = w_vocab.shape[1]
        v_own = v_tp // n2
        chunks = rows // ROWS
        half = d_local // 2
        n_x = n1 // 2
        blk = ROWS // n_x
        pack = min(2, chunks)
        thirds = 3 if ff_own % 48 == 0 else 1
        window = -(-v_own // 16) * 16
        part = v_own - (v_own // 2) // 8 * 8
        bf, f32 = jnp.bfloat16, jnp.float32
        n_loads = -(-chunks // pack) + thirds + 2 + 3 + 5
        n_arrivals = 9 + 12 * (chunks - 1) + 2
        row = lambda a: a.reshape(1, -1)
        vmem = pl.BlockSpec(memory_space=pltpu.VMEM)
        hbm = pl.BlockSpec(memory_space=pl.ANY)
        results = [
            jax.ShapeDtypeStruct((1, rows), f32),
            jax.ShapeDtypeStruct((1, rows), f32),
            jax.ShapeDtypeStruct((1, rows), f32),
            jax.ShapeDtypeStruct((v_own, rows), bf),
        ]
        parts = pl.pallas_call(
            functools.partial(kernel, n2, n1, pack),
            out_shape=results,
            in_specs=[hbm] * 8,
            out_specs=[hbm] * 4,
            scratch_shapes=[
                pltpu.VMEM((chunks, ROWS, d_model), bf),
                pltpu.VMEM((thirds, 2 * ff_own // thirds, d_model), bf),
                pltpu.VMEM((ff_tp, d_local), bf),
                pltpu.VMEM((v_tp, d_local), bf),
                pltpu.VMEM((chunks, ff_tp, ROWS), bf),
                pltpu.VMEM((chunks, 2, ROWS, half), bf),
                pltpu.VMEM((chunks, ROWS, half), bf),
                pltpu.VMEM((chunks, ROWS, half), bf),
                pltpu.VMEM((chunks, n_x - 1, blk, half), bf),
                pltpu.VMEM((chunks, 2, ROWS, half), bf),
                pltpu.VMEM((chunks, n2, 8, ROWS), f32),
                pltpu.VMEM((chunks, ROWS, d_local), bf),
                pltpu.VMEM((chunks, n2, window, ROWS), f32),
                pltpu.VMEM((chunks, 2, part, ROWS), f32),
                pltpu.VMEM((chunks, 2, part, ROWS), f32),
                pltpu.VMEM((chunks, 2, part, ROWS), f32),
                pltpu.VMEM((ROWS, LANES), f32),
                pltpu.VMEM((n2 * n1, 8, ROWS), f32),
                pltpu.VMEM((n1, 4, 1, rows - ROWS), f32),
                pltpu.VMEM((n2, 4, 1, rows - ROWS), f32),
                pltpu.VMEM((n2 * n1, 4, 1, ROWS), f32),
                pltpu.VMEM((1, d_model), f32),
                pltpu.VMEM((1, rows), f32),
                pltpu.VMEM((1, rows), jnp.int32),
                pltpu.VMEM((1, rows), f32),
                pltpu.VMEM((1, rows), f32),
                pltpu.VMEM((1, rows), f32),
                pltpu.VMEM((v_own, rows), bf),
                pltpu.SemaphoreType.DMA((n_loads,)),
                pltpu.SemaphoreType.DMA((9,)),
                pltpu.SemaphoreType.DMA((n_arrivals,)),
                pltpu.SemaphoreType.DMA((2, 2)),
            ],
            compiler_params=pltpu.CompilerParams(
                collective_id=0, has_side_effects=True, vmem_limit_bytes=66_000_000,
            ),
            name="decode_tail",
        )(
            hidden, w_gate.T, w_up.T, w_down, row(norm_gain), w_vocab.T,
            row(temperature), row(target),
        )
        ln, ent, tgt, lp = pl.pallas_call(
            emit, out_shape=results, in_specs=[hbm] * 4, out_specs=[hbm] * 4,
            scratch_shapes=[pltpu.VMEM(r.shape, r.dtype) for r in results]
            + [pltpu.SemaphoreType.DMA((2, 7))],
            name="emit",
        )(*parts)
        return ln.reshape(rows), ent.reshape(rows), tgt.reshape(rows), lp.T

    return jax.shard_map(
        device_step, mesh=mesh,
        in_specs=(
            P("dp", None), P(None, ("tp", "tp2")), P(None, ("tp", "tp2")), P("tp", "tp2"),
            P(None), P("tp2", "tp"), P("dp"), P("dp"),
        ),
        out_specs=(P("dp"), P("dp"), P("dp"), P("dp", ("tp", "tp2"))),
        check_vma=False,
    )
```

```python
import functools

import jax
import jax.numpy as jnp
from jax import lax
from jax.experimental import pallas as pl
from jax.experimental.pallas import tpu as pltpu
from jax.sharding import PartitionSpec as P

NORM_EPS = 1e-6
ROWS = 128
LANES = 128
MESH = pl.DeviceIdType.MESH


class Sems:
    def __init__(self, ref):
        self.ref, self.used = ref, 0

    def take(self):
        self.used += 1
        return self.ref.at[self.used - 1]


def kernel(
    n2, n1, pack,
    hidden, w_gate, w_up, w_down, gain_in, w_vocab, temp_in, target_in,
    out_ln, out_ent, out_tgt, out_lp,
    hid, wgu, wd, wv, act_t, yp, pair, chip, xr, ys, sq, xs,
    lg, far, mrg, dct, sq_col, sq_all, st_a, st_y, st_b, gain, temp, target, ln, ent, tgt_lp, lp_out,
    load_sems, send_sems, recv_sems, cast_sems,
):
    chunks, _, d_model = hid.shape
    thirds, ff_part = wgu.shape[0], wgu.shape[1] // 2
    ff_own = thirds * ff_part
    d_local = wd.shape[1]
    half = d_local // 2
    v_own = out_lp.shape[0]
    n_x = n1 // 2
    blk = ROWS // n_x
    y = lax.axis_index("tp2")
    tp = lax.axis_index("tp")
    x, core = tp // 2, tp % 2
    loads = Sems(load_sems)
    send_ids, recv_ids = {}, {}

    def at_y(j):
        return {"tp2": (y + j) % n2}

    def at_x(j):
        return {"tp": ((x + j) % n_x) * 2 + core}

    partner = {"tp": x * 2 + (1 - core)}

    def remote(src, dst, device, out, into):
        return pltpu.make_async_remote_copy(
            src_ref=src, dst_ref=dst,
            send_sem=send_sems.at[send_ids.setdefault(out, len(send_ids))],
            recv_sem=recv_sems.at[recv_ids.setdefault(into, len(recv_ids))],
            device_id=device, device_id_type=MESH,
        )

    def send(copy):
        copy.start()

    def arrived(into, amount):
        pltpu.make_async_copy(amount, amount, recv_sems.at[recv_ids[into]]).wait()

    everyone = sorted(
        [(j2, j1) for j2 in range(n2) for j1 in range(n1)][1:],
        key=lambda j: -min(j[0], n2 - j[0]) - min(j[1] // 2, n_x - j[1] // 2),
    )

    def slot_of(y_from, tp_from):
        return ((y + n2 - y_from) % n2) * n1 + (tp + n1 - tp_from) % n1

    def broadcast(buf, index):
        for j2, j1 in everyone:
            pltpu.make_async_remote_copy(
                src_ref=buf.at[0], dst_ref=buf.at[j2 * n1 + j1],
                send_sem=cast_sems.at[index, 0], recv_sem=cast_sems.at[index, 1],
                device_id={"tp2": (y + j2) % n2, "tp": (tp + j1) % n1}, device_id_type=MESH,
            ).start()

    def wait_cast(buf, index, side):
        rest = buf.at[pl.ds(1, n2 * n1 - 1)]
        pltpu.make_async_copy(rest, rest, cast_sems.at[index, side]).wait()

    ff_cut = (ff_own // 2) // 16 * 16
    v_cut = (v_own // 2) // 8 * 8

    def act_rows(i, q, lo, size):
        return act_t.at[i, pl.ds(pl.multiple_of(q * ff_own + lo, 16), size), :]

    def q_of(slot):
        return (y + slot) % n2

    def base_of(slot):
        return pl.multiple_of((v_own * q_of(slot)) // 16 * 16, 16)

    def off_of(slot):
        return pl.multiple_of((v_own * q_of(slot)) % 16, 8)

    def lg_part(i, slot, part):
        lo, size = (0, v_cut) if part == 0 else (v_cut, v_own - v_cut)
        return lg.at[i, slot, pl.ds(pl.multiple_of(off_of(slot) + lo, 8), size), :]

    def part_of(buf, i, part):
        return buf.at[i, part, pl.ds(0, v_cut if part == 0 else v_own - v_cut), :]

    def pieces(i, slot, part, buf):
        lo, size = (0, v_cut) if part == 0 else (v_cut, v_own - v_cut)
        cut = size // 2 // 8 * 8 if i == 0 else size
        for at, n in ((0, cut), (cut, size - cut)):
            if n > 0:
                src = pl.ds(pl.multiple_of(off_of(slot) + lo + at, 8), n)
                yield lg.at[i, slot, src, :], buf.at[i, part, pl.ds(at, n), :]

    x_order = [n_x // 2] + [j for j in range(1, n_x) if j != n_x // 2]

    cps = []
    for i in range(chunks):
        c = {}
        parts = thirds if i == 0 else 1
        own = [act_rows(i, y, t * (ff_own // parts), ff_own // parts) for t in range(parts)]
        up, dn = ("act", "act") if i == 0 else ("up", "dn")
        c["own_up"] = [remote(a, a, at_y(1), "act", (up, i)) for a in own]
        c["own_dn"] = [remote(a, a, at_y(-1), "act", (dn, i)) for a in own]
        prev, nxt = (y + n2 - 1) % n2, (y + 1) % n2
        if i == 0:
            c["own_far"] = [remote(a, a, at_y(2), "act", (up, i)) for a in own]
        else:
            lo_half = act_rows(i, prev, 0, ff_cut)
            hi_half = act_rows(i, nxt, ff_cut, ff_own - ff_cut)
            c["fwd_up"] = remote(lo_half, lo_half, at_y(1), "act", ("fwd", i))
            c["fwd_dn"] = remote(hi_half, hi_half, at_y(-1), "act", ("fwd", i))
        c["pair"] = remote(yp.at[i, 1 - core], pair.at[i], partner, "pair", ("pair", i))
        c["xrs"] = [
            remote(
                chip.at[i, pl.ds(pl.multiple_of(((x + j) % n_x) * blk, blk), blk), :],
                xr.at[i, j - 1], at_x(j), "xrs", ("xrs", i),
            )
            for j in x_order
        ]
        mine = ys.at[i, core, pl.ds(pl.multiple_of(x * blk, blk), blk), :]
        c["xag"] = [remote(mine, mine, at_x(j), "xag", ("xag", i)) for j in x_order]
        c["swap"] = remote(ys.at[i, core], ys.at[i, core], partner, "swap", ("swap", i))
        c["ssq"] = [] if i == 0 else [
            remote(sq.at[i, 0], sq.at[i, j], at_y(j), "ssq", ("ssq", i)) for j in range(1, n2)
        ]
        for name, slot, part, buf, way in (
            ("far_a", 2, 0, far, -1), ("far_b", 2, 1, far, 1),
            ("mrg_a", 3, 0, mrg, -1), ("mrg_b", 1, 1, mrg, 1),
        ):
            into = name if buf is far else "mrg"
            c[name] = remote(lg_part(i, slot, part), part_of(buf, i, part), at_y(way), "lg", (into, i))
        for name, slot, part, way in (("dir_a", 1, 0, 1), ("dir_b", 3, 1, -1)):
            c[name] = [remote(a, b, at_y(way), "lg", ("dir", i)) for a, b in pieces(i, slot, part, dct)]
        cps.append(c)
    cp_tp = [
        remote(st_a.at[0], st_a.at[j], {"tp": (tp + j) % n1}, "tp", "tp") for j in range(n1 - 1, 0, -1)
    ]
    cp_y = [remote(st_y.at[0], st_y.at[j], at_y(j), "y", "y") for j in range(1, n2)]
    all_sent = {
        "act": act_t.at[:, pl.ds(0, (n2 - 1) * ff_own), :], "pair": pair, "xrs": xr, "xag": xr, "swap": pair,
        "ssq": sq.at[pl.ds(1, chunks - 1), pl.ds(1, n2 - 1)],
        "lg": lg.at[:, pl.ds(0, 3), pl.ds(0, v_own), :],
        "tp": st_a.at[pl.ds(1, n1 - 1)], "y": st_y.at[pl.ds(1, n2 - 1)],
    }

    def load(src, dst):
        return pltpu.make_async_copy(src, dst, loads.take())

    def load_columns(src, dst, parts):
        cols, sem = d_model // parts, loads.take()
        cps = [
            pltpu.make_async_copy(a.at[:, pl.ds(k * cols, cols)], b.at[:, pl.ds(k * cols, cols)], sem)
            for k in range(parts) for a, b in zip(src, dst)
        ]
        return cps, sem

    ld_hid = [
        load_columns(
            [hidden.at[pl.ds(j * ROWS, ROWS), :] for j in range(i, i + pack)],
            [hid.at[j] for j in range(i, i + pack)], 1,
        )
        for i in range(0, chunks, pack)
    ]
    ld_w = [
        load_columns(
            [w.at[pl.ds(t * ff_part, ff_part), :] for w in (w_gate, w_up)],
            [wgu.at[t, pl.ds(side * ff_part, ff_part), :] for side in range(2)],
            5 if d_model % (5 * LANES) == 0 else 4,
        )
        for t in range(thirds)
    ]

    def wait_load(group, dst):
        pltpu.make_async_copy(dst, dst, group[1]).wait()

    ld_wd = load(w_down, wd)
    ld_wv = load(w_vocab, wv)
    ld_small = [load(gain_in, gain), load(temp_in, temp), load(target_in, target)]
    peers = [{"tp2": (y + j2) % n2, "tp": (tp + j1) % n1} for j2, j1 in everyone]
    with jax.named_scope("start"):
        for cp in [cp for group in [ld_hid[0]] + ld_w for cp in group[0]]:
            cp.start()
        for cp in ld_small:
            cp.start()
        barrier = pltpu.get_barrier_semaphore()
        for device in peers:
            pl.semaphore_signal(barrier, inc=1, device_id=device, device_id_type=MESH)

    NT = (((1,), (1,)), ((), ()))

    def gate_up(first, t):
        r = lax.dot_general(
            wgu[t], hid[first:first + pack].reshape(pack * ROWS, d_model), NT,
            preferred_element_type=jnp.float32,
        )
        act = (jax.nn.silu(r[:ff_part]) * r[ff_part:]).astype(jnp.bfloat16)
        for i in range(pack):
            at = pl.ds(pl.multiple_of(y * ff_own + t * ff_part, 16), ff_part)
            act_t[first + i, at, :] = act[:, i * ROWS:(i + 1) * ROWS]

    def send_own(i, t=0):
        send(cps[i]["own_up"][t])
        if i == 0:
            send(cps[i]["own_far"][t])
        send(cps[i]["own_dn"][t])

    def forward(i):
        amount = act_t.at[i, pl.ds(0, ff_own), :]
        arrived(("up", i), amount)
        send(cps[i]["fwd_up"])
        arrived(("dn", i), amount)
        send(cps[i]["fwd_dn"])

    def down(i):
        name, count = ("act", n2 - 1) if i == 0 else ("fwd", 1)
        arrived((name, i), act_t.at[i, pl.ds(0, count * ff_own), :])
        if i == 0:
            ld_wd.wait()
        for s in range(2):
            yp[i, s] = lax.dot_general(
                act_t[i], wd[:, s * half:(s + 1) * half],
                (((0,), (0,)), ((), ())), preferred_element_type=jnp.float32,
            ).astype(jnp.bfloat16)
        send(cps[i]["pair"])

    def chip_sum(i):
        arrived(("pair", i), pair.at[i])
        chip[i] = (
            yp[i, core].astype(jnp.float32) + pair[i].astype(jnp.float32)
        ).astype(jnp.bfloat16)
        for cp in cps[i]["xrs"]:
            send(cp)

    def row_sum(i):
        at = pl.ds(pl.multiple_of(x * blk, blk), blk)
        total = chip[i, at, :].astype(jnp.float32)
        arrived(("xrs", i), xr.at[i])
        for j in x_order:
            total += xr[i, j - 1].astype(jnp.float32)
        total = total.astype(jnp.bfloat16)
        ys[i, core, at, :] = total
        for cp in cps[i]["xag"]:
            send(cp)
        if i == 0:
            cols = pl.ds(pl.multiple_of(y * d_local + core * half, LANES), half)
            r = hid[i, at, cols].astype(jnp.float32) + total.astype(jnp.float32)
            part = jnp.sum(r * r, axis=1, keepdims=True)
            sq_col[...] = jnp.zeros_like(sq_col)
            sq_col[at, :] = jnp.broadcast_to(part, (blk, LANES))
            sq_all[0] = sq_col[...].T[:8, :]
            broadcast(sq_all, 0)

    def swap(i):
        arrived(("xag", i), xr.at[i])
        send(cps[i]["swap"])

    def residual(i, s):
        cols = pl.ds(pl.multiple_of(y * d_local + s * half, LANES), half)
        return hid[i, :, cols].astype(jnp.float32) + ys[i, s].astype(jnp.float32)

    def square(i):
        arrived(("swap", i), pair.at[i])
        part = 0.0
        for s in range(2):
            r = residual(i, s)
            part = part + jnp.sum(r * r, axis=1, keepdims=True)
        sq[i, 0] = jnp.broadcast_to(part, (ROWS, LANES)).T[:8, :]
        for cp in cps[i]["ssq"]:
            send(cp)

    def norm(i):
        if i == 0:
            arrived(("swap", i), pair.at[i])
            wait_cast(sq_all, 0, 1)
            total = jnp.sum(sq_all[...], axis=0)
        else:
            total = sq[i, 0]
            arrived(("ssq", i), sq.at[i, pl.ds(1, n2 - 1)])
            for j in range(1, n2):
                total = total + sq[i, j]
        inv = lax.rsqrt(total / d_model + NORM_EPS)
        inv = jnp.broadcast_to(inv[:1, :], (LANES, ROWS)).T[:, :1]
        for s in range(2):
            g = gain[:, pl.ds(pl.multiple_of(y * d_local + s * half, LANES), half)]
            xs[i, :, s * half:(s + 1) * half] = (g * residual(i, s) * inv).astype(jnp.bfloat16)

    window = lg.shape[2]
    step = window // 3 if window % 48 == 0 else window

    def piece(i, slot, at, size):
        lg[i, slot, pl.ds(at, size), :] = lax.dot_general(
            wv[pl.ds(pl.multiple_of(base_of(slot) + at, 16), size), :], xs[i], NT,
            preferred_element_type=jnp.float32,
        )

    def logits(i, slot):
        @pl.loop(0, window // step)
        def _(j):
            piece(i, slot, pl.multiple_of(j * step, 16), step)

    def logits_far(i):
        if i == 0:
            cut = -(-(v_cut + 8) // 16) * 16
            piece(i, 2, 0, cut)
            send(cps[i]["far_a"])
            piece(i, 2, cut, window - cut)
        else:
            logits(i, 2)
            send(cps[i]["far_a"])
        send(cps[i]["far_b"])

    def logits_up(i):
        logits(i, 1)
        send(cps[i]["dir_a"][0])

    def logits_down(i):
        logits(i, 3)
        send(cps[i]["dir_b"][0])

    def near_send(i):
        send(cps[i]["dir_a"][1])
        send(cps[i]["dir_b"][1])

    def merge(i):
        for name, slot, part in (("a", 3, 0), ("b", 1, 1)):
            arrived(("far_" + name, i), part_of(far, i, part))
            lg_part(i, slot, part)[...] += part_of(far, i, part)[...]
            send(cps[i]["mrg_" + name])

    def own(i):
        logits(i, 0)

    def near_sum(i):
        arrived(("dir", i), lg.at[i, 0, pl.ds(0, v_own), :])
        for part in range(2):
            lg_part(i, 0, part)[...] += part_of(dct, i, part)[...]

    def finish(i):
        lanes = pl.ds(i * ROWS, ROWS)
        t = temp[:, lanes]
        tgt = target[:, lanes]
        col0 = (tp * n2 + y) * v_own
        peak = None
        arrived(("mrg", i), lg.at[i, 0, pl.ds(0, v_own), :])
        for part in range(2):
            ref = lg_part(i, 0, part)
            val = (ref[...] + part_of(mrg, i, part)[...]) / t
            ref[...] = val
            top = jnp.max(val, axis=0, keepdims=True)
            peak = top if peak is None else jnp.maximum(peak, top)
        total = dot = hit = 0.0
        for part in range(2):
            val = lg_part(i, 0, part)[...]
            e = jnp.exp(val - peak)
            total = total + jnp.sum(e, axis=0, keepdims=True)
            dot = dot + jnp.sum(e * val, axis=0, keepdims=True)
            ids = col0 + part * v_cut + lax.broadcasted_iota(jnp.int32, val.shape, 0)
            hit = hit + jnp.sum(jnp.where(ids == tgt, val, 0.0), axis=0, keepdims=True)
        buf, at = (st_b, slice(0, ROWS)) if i == chunks - 1 else (st_a, lanes)
        for row, v in enumerate((peak, total, dot, hit)):
            buf[0, row, :, at] = v

    def combine(buf, slots):
        peak = jnp.max(buf[:, 0], axis=0)
        total = dot = hit = 0.0
        for slot in slots:
            v = buf[slot]
            scale = jnp.exp(v[0] - peak)
            total = total + v[1] * scale
            dot = dot + v[2] * scale
            hit = hit + v[3]
        return peak, total, dot, hit

    def row_results(stats, lanes):
        peak, total, dot, hit = stats
        log_norm = peak + jnp.log(total)
        ln[:, lanes] = log_norm
        ent[:, lanes] = log_norm - dot / total
        tgt_lp[:, lanes] = hit - log_norm

    def output(first, count):
        for i in range(first, first + count):
            lanes = slice(i * ROWS, (i + 1) * ROWS)
            val = lg[i, 0, pl.ds(off_of(0), v_own), :]
            lp_out[:, lanes] = (val - ln[:, lanes]).astype(jnp.bfloat16)

    last = chunks - 1

    def run(*items):
        for fn, i in items:
            if 0 <= i <= last:
                with jax.named_scope(f"{fn.__name__}#c={i}"):
                    fn(i)

    wait_load(ld_hid[0], hid.at[pl.ds(0, pack)])
    for t in range(thirds):
        with jax.named_scope(f"gate_up#c=0#t={t}"):
            wait_load(ld_w[t], wgu.at[t])
            if t == thirds - 1:
                for cp in [cp for group in ld_hid[1:] for cp in group[0]]:
                    cp.start()
            gate_up(0, t)
        if t == 0:
            with jax.named_scope("barrier"):
                pl.semaphore_wait(barrier, len(peers))
        send_own(0, t)
    ld_wd.start()
    for i in range(1, pack):
        send_own(i)
    ld_wv.start()
    for i in range(pack, chunks, pack):
        wait_load(ld_hid[i // pack], hid.at[pl.ds(i, pack)])
        with jax.named_scope(f"gate_up#c={i}"):
            for t in range(thirds):
                gate_up(i, t)
    for cp in ld_small:
        cp.wait()
    run((send_own, 2), (down, 0), (chip_sum, 0), (forward, 1), (row_sum, 0), (send_own, 3))
    run((forward, 2), (down, 1), (swap, 0), (chip_sum, 1), (norm, 0), (forward, 3))
    ld_wv.wait()
    run((logits_far, 0), (logits_up, 0), (row_sum, 1), (logits_down, 0), (down, 2), (down, 3), (chip_sum, 2))
    run((chip_sum, 3), (swap, 1), (square, 1), (near_send, 0), (row_sum, 2), (norm, 1))
    run((logits_far, 1), (row_sum, 3), (swap, 2), (square, 2), (merge, 0), (logits_up, 1), (logits_down, 1))
    run((swap, 3), (square, 3), (norm, 2))
    for i in range(1, chunks - 1):
        run((logits_far, i + 1), (merge, i), (logits_up, i + 1), (logits_down, i + 1), (norm, i + 2))
        run((own, i - 1), (near_sum, i - 1))
    run((finish, last - 3), (own, last - 1), (own, last), (near_sum, last - 1), (finish, last - 2))
    run((merge, last), (finish, last - 1))
    for cp in cp_tp:
        send(cp)
    run((near_sum, last),)
    with jax.named_scope("stats_tp"):
        arrived("tp", st_a.at[pl.ds(1, n1 - 1)])
        for row, v in enumerate(combine(st_a, [(tp + n1 - j) % n1 for j in range(n1)])):
            st_y[0, row] = v
        for cp in cp_y:
            send(cp)
    run((finish, last),)
    with jax.named_scope("cast_b"):
        broadcast(st_b, 1)
    with jax.named_scope("output_a"):
        arrived("y", st_y.at[pl.ds(1, n2 - 1)])
        row_results(combine(st_y, [(y + n2 - j) % n2 for j in range(n2)]), slice(0, last * ROWS))
        output(0, last)
        first_store = load(lp_out.at[:, :last * ROWS], out_lp.at[:, :last * ROWS])
        first_store.start()
    with jax.named_scope("sent"):
        for out, amount in all_sent.items():
            pltpu.make_async_copy(amount, amount, send_sems.at[send_ids[out]]).wait()
        wait_cast(sq_all, 0, 0)
    with jax.named_scope("wait_b"):
        wait_cast(st_b, 1, 1)
    with jax.named_scope("output_b"):
        order = [slot_of(j2, j1) for j2 in range(n2) for j1 in range(n1)]
        row_results(combine(st_b, order), slice(last * ROWS, chunks * ROWS))
        output(last, 1)
    with jax.named_scope("drain"):
        stores = [load(lp_out.at[:, last * ROWS:], out_lp.at[:, last * ROWS:])]
        stores += [load(a, b) for a, b in ((ln, out_ln), (ent, out_ent), (tgt_lp, out_tgt))]
        for cp in stores:
            cp.start()
        wait_cast(st_b, 1, 0)
        for cp in [first_store] + stores:
            cp.wait()


def emit(*refs):
    ins, outs, bufs, sems = refs[:4], refs[4:8], refs[8:12], refs[12]
    rows = ins[3].shape[0]
    cut = -(-rows // 64) * 16
    pieces = [(3, pl.ds(lo, min(cut, rows - lo))) for lo in range(0, rows, cut)]
    pieces += [(n, pl.ds(0, 1)) for n in range(3)]
    taken = [
        pltpu.make_async_copy(ins[n].at[at, :], bufs[n].at[at, :], sems.at[0, k])
        for k, (n, at) in enumerate(pieces)
    ]
    given = [
        pltpu.make_async_copy(bufs[n].at[at, :], outs[n].at[at, :], sems.at[1, k])
        for k, (n, at) in enumerate(pieces)
    ]
    for cp in taken:
        cp.start()
    for a, b in zip(taken, given):
        a.wait()
        b.start()
    for cp in given:
        cp.wait()


def solution(mesh):
    n2, n1 = mesh.shape["tp2"], mesh.shape["tp"]

    def device_step(hidden, w_gate, w_up, w_down, norm_gain, w_vocab, temperature, target):
        rows, d_model = hidden.shape
        ff_own = w_gate.shape[1]
        ff_tp, d_local = w_down.shape
        v_tp = w_vocab.shape[1]
        v_own = v_tp // n2
        chunks = rows // ROWS
        half = d_local // 2
        n_x = n1 // 2
        blk = ROWS // n_x
        pack = min(2, chunks)
        thirds = 3 if ff_own % 48 == 0 else 1
        window = -(-v_own // 16) * 16
        part = v_own - (v_own // 2) // 8 * 8
        bf, f32 = jnp.bfloat16, jnp.float32
        n_loads = -(-chunks // pack) + thirds + 2 + 3 + 5
        n_arrivals = 9 + 12 * (chunks - 1) + 2
        row = lambda a: a.reshape(1, -1)
        vmem = pl.BlockSpec(memory_space=pltpu.VMEM)
        hbm = pl.BlockSpec(memory_space=pl.ANY)
        results = [
            jax.ShapeDtypeStruct((1, rows), f32),
            jax.ShapeDtypeStruct((1, rows), f32),
            jax.ShapeDtypeStruct((1, rows), f32),
            jax.ShapeDtypeStruct((v_own, rows), bf),
        ]
        parts = pl.pallas_call(
            functools.partial(kernel, n2, n1, pack),
            out_shape=results,
            in_specs=[hbm] * 8,
            out_specs=[hbm] * 4,
            scratch_shapes=[
                pltpu.VMEM((chunks, ROWS, d_model), bf),
                pltpu.VMEM((thirds, 2 * ff_own // thirds, d_model), bf),
                pltpu.VMEM((ff_tp, d_local), bf),
                pltpu.VMEM((v_tp, d_local), bf),
                pltpu.VMEM((chunks, ff_tp, ROWS), bf),
                pltpu.VMEM((chunks, 2, ROWS, half), bf),
                pltpu.VMEM((chunks, ROWS, half), bf),
                pltpu.VMEM((chunks, ROWS, half), bf),
                pltpu.VMEM((chunks, n_x - 1, blk, half), bf),
                pltpu.VMEM((chunks, 2, ROWS, half), bf),
                pltpu.VMEM((chunks, n2, 8, ROWS), f32),
                pltpu.VMEM((chunks, ROWS, d_local), bf),
                pltpu.VMEM((chunks, n2, window, ROWS), f32),
                pltpu.VMEM((chunks, 2, part, ROWS), f32),
                pltpu.VMEM((chunks, 2, part, ROWS), f32),
                pltpu.VMEM((chunks, 2, part, ROWS), f32),
                pltpu.VMEM((ROWS, LANES), f32),
                pltpu.VMEM((n2 * n1, 8, ROWS), f32),
                pltpu.VMEM((n1, 4, 1, rows - ROWS), f32),
                pltpu.VMEM((n2, 4, 1, rows - ROWS), f32),
                pltpu.VMEM((n2 * n1, 4, 1, ROWS), f32),
                pltpu.VMEM((1, d_model), f32),
                pltpu.VMEM((1, rows), f32),
                pltpu.VMEM((1, rows), jnp.int32),
                pltpu.VMEM((1, rows), f32),
                pltpu.VMEM((1, rows), f32),
                pltpu.VMEM((1, rows), f32),
                pltpu.VMEM((v_own, rows), bf),
                pltpu.SemaphoreType.DMA((n_loads,)),
                pltpu.SemaphoreType.DMA((9,)),
                pltpu.SemaphoreType.DMA((n_arrivals,)),
                pltpu.SemaphoreType.DMA((2, 2)),
            ],
            compiler_params=pltpu.CompilerParams(
                collective_id=0, has_side_effects=True, vmem_limit_bytes=66_000_000,
            ),
            name="decode_tail",
        )(
            hidden, w_gate.T, w_up.T, w_down, row(norm_gain), w_vocab.T,
            row(temperature), row(target),
        )
        ln, ent, tgt, lp = pl.pallas_call(
            emit, out_shape=results, in_specs=[hbm] * 4, out_specs=[hbm] * 4,
            scratch_shapes=[pltpu.VMEM(r.shape, r.dtype) for r in results]
            + [pltpu.SemaphoreType.DMA((2, 7))],
            name="emit",
        )(*parts)
        return ln.reshape(rows), ent.reshape(rows), tgt.reshape(rows), lp.T

    return jax.shard_map(
        device_step, mesh=mesh,
        in_specs=(
            P("dp", None), P(None, ("tp", "tp2")), P(None, ("tp", "tp2")), P("tp", "tp2"),
            P(None), P("tp2", "tp"), P("dp"), P("dp"),
        ),
        out_specs=(P("dp"), P("dp"), P("dp"), P("dp", ("tp", "tp2"))),
        check_vma=False,
    )
```
